32 devices in a mesh: dp: 4 (over y, z), tp: 8 (over x, core).
Axes of the slice: x: 4, y: 2, z: 2, core: 2. Of those that a mesh axis runs over, the one named last changes fastest.
The devices are a block of a 4x4x8 slice.
Arguments:
- x_in: bfloat16 [32, 256, 4096], P('dp'), parts along dimension 0
- adapter_ids: int32 [32], P('dp'), parts along dimension 0
- gain_attn: float32 [4096], replicated
- gain_mlp: float32 [4096], replicated
- w_q: bfloat16 [4096, 32, 128], P(None, 'tp')
- w_k: bfloat16 [4096, 8, 128], P(None, 'tp')
- w_v: bfloat16 [4096, 8, 128], P(None, 'tp')
- w_o: bfloat16 [32, 128, 4096], P('tp')
- w_gate: bfloat16 [4096, 14336], P(None, 'tp')
- w_up: bfloat16 [4096, 14336], P(None, 'tp')
- w_down: bfloat16 [14336, 4096], P('tp')
- a_q: bfloat16 [8, 4096, 8], P(None, None, 'tp')
- b_q: bfloat16 [8, 8, 32, 128], P(None, None, 'tp')
- a_k: bfloat16 [8, 4096, 8], P(None, None, 'tp')
- b_k: bfloat16 [8, 8, 8, 128], P(None, None, 'tp')
- a_v: bfloat16 [8, 4096, 8], P(None, None, 'tp')
- b_v: bfloat16 [8, 8, 8, 128], P(None, None, 'tp')
- a_o: bfloat16 [8, 32, 128, 8], P(None, 'tp')
- b_o: bfloat16 [8, 8, 4096], P(None, None, 'tp')
- a_gate: bfloat16 [8, 4096, 8], P(None, None, 'tp')
- b_gate: bfloat16 [8, 8, 14336], P(None, None, 'tp')
- a_up: bfloat16 [8, 4096, 8], P(None, None, 'tp')
- b_up: bfloat16 [8, 8, 14336], P(None, None, 'tp')
- a_down: bfloat16 [8, 14336, 8], P(None, 'tp')
- b_down: bfloat16 [8, 8, 4096], P(None, None, 'tp')
Outputs:
- output: bfloat16 [32, 256, 4096], P('dp'), parts along dimension 0
There are 4 independent parts. The reference program is written for one: setup_inputs(seed, part) draws one part's arguments, and reference() takes and returns one part's arrays. A program takes and returns all parts, laid end to end along the dimension named above; an argument that names none is the same for every part.
All inputs are finite; a program needn't handle non-finite values.
Results may differ from the reference program's by a relative error of at most 0.02.
Values are sent between devices in bfloat16 or wider.
A program may use at most 768 MiB of HBM per device.

```python
import jax
import jax.numpy as jnp
from jax import lax

BATCH = 8
SEQ_LEN = 256
D_MODEL = 4096
HEADS = 32
KV_HEADS = 8
HEAD_DIM = 128
D_FF = 14336
RANK = 8
ADAPTERS = 8
LORA_ALPHA = 16
RMS_EPS = 1e-5
Q_WIDTH = HEADS * HEAD_DIM
KV_WIDTH = KV_HEADS * HEAD_DIM


def draw_normal(rng_key, arr_shape, w_std):
    return (jax.random.normal(rng_key, arr_shape, jnp.float32) * w_std).astype(jnp.bfloat16)


def lora_pair(rng_key, a_shape, b_shape, fan_in, w_gain):
    key_a, key_b = jax.random.split(rng_key)
    a_stack = draw_normal(key_a, a_shape, fan_in ** -0.5)
    b_stack = draw_normal(key_b, b_shape, 0.2 * w_gain * RANK ** 0.5 / LORA_ALPHA)
    return a_stack, b_stack


def draw_ids(rng_key):
    key_perm, key_fill, key_mix = jax.random.split(rng_key, 3)
    id_perm = jax.random.permutation(key_perm, ADAPTERS).astype(jnp.int32)
    id_fill = jax.random.randint(key_fill, (BATCH,), 0, ADAPTERS).astype(jnp.int32)
    id_all = jnp.concatenate([id_perm, id_fill])[:BATCH]
    return jax.random.permutation(key_mix, id_all).astype(jnp.int32)


def setup_inputs(seed: int = 0, part: int = 0) -> dict:
    root_key = jax.random.key(seed)
    key_x, key_ids = jax.random.split(jax.random.fold_in(root_key, part))
    shared_keys = jax.random.split(root_key, 16)
    x_in = (0.5 * jax.random.normal(key_x, (BATCH, SEQ_LEN, D_MODEL), jnp.float32)).astype(jnp.bfloat16)
    gain_attn = 1.0 + 0.2 * jax.random.normal(shared_keys[0], (D_MODEL,), jnp.float32)
    gain_mlp = 1.0 + 0.2 * jax.random.normal(shared_keys[1], (D_MODEL,), jnp.float32)
    w_q = draw_normal(shared_keys[2], (D_MODEL, HEADS, HEAD_DIM), 1.7 * D_MODEL ** -0.5)
    w_k = draw_normal(shared_keys[3], (D_MODEL, KV_HEADS, HEAD_DIM), 1.7 * D_MODEL ** -0.5)
    w_v = draw_normal(shared_keys[4], (D_MODEL, KV_HEADS, HEAD_DIM), D_MODEL ** -0.5)
    w_o = draw_normal(shared_keys[5], (HEADS, HEAD_DIM, D_MODEL), Q_WIDTH ** -0.5)
    w_gate = draw_normal(shared_keys[6], (D_MODEL, D_FF), D_MODEL ** -0.5)
    w_up = draw_normal(shared_keys[7], (D_MODEL, D_FF), D_MODEL ** -0.5)
    w_down = draw_normal(shared_keys[8], (D_FF, D_MODEL), D_FF ** -0.5)
    a_q, b_q = lora_pair(shared_keys[9], (ADAPTERS, D_MODEL, RANK), (ADAPTERS, RANK, HEADS, HEAD_DIM), D_MODEL, 1.7)
    a_k, b_k = lora_pair(shared_keys[10], (ADAPTERS, D_MODEL, RANK), (ADAPTERS, RANK, KV_HEADS, HEAD_DIM), D_MODEL, 1.7)
    a_v, b_v = lora_pair(shared_keys[11], (ADAPTERS, D_MODEL, RANK), (ADAPTERS, RANK, KV_HEADS, HEAD_DIM), D_MODEL, 1.0)
    a_o, b_o = lora_pair(shared_keys[12], (ADAPTERS, HEADS, HEAD_DIM, RANK), (ADAPTERS, RANK, D_MODEL), Q_WIDTH, 1.0)
    a_gate, b_gate = lora_pair(shared_keys[13], (ADAPTERS, D_MODEL, RANK), (ADAPTERS, RANK, D_FF), D_MODEL, 1.0)
    a_up, b_up = lora_pair(shared_keys[14], (ADAPTERS, D_MODEL, RANK), (ADAPTERS, RANK, D_FF), D_MODEL, 1.0)
    a_down, b_down = lora_pair(shared_keys[15], (ADAPTERS, D_FF, RANK), (ADAPTERS, RANK, D_MODEL), D_FF, 1.0)
    return dict(x_in=x_in, adapter_ids=draw_ids(key_ids), gain_attn=gain_attn, gain_mlp=gain_mlp,
                w_q=w_q, w_k=w_k, w_v=w_v, w_o=w_o, w_gate=w_gate, w_up=w_up, w_down=w_down,
                a_q=a_q, b_q=b_q, a_k=a_k, b_k=b_k, a_v=a_v, b_v=b_v, a_o=a_o, b_o=b_o,
                a_gate=a_gate, b_gate=b_gate, a_up=a_up, b_up=b_up, a_down=a_down, b_down=b_down)


def rms_scale(x_in, gain_vec):
    x_f32 = x_in.astype(jnp.float32)
    inv_rms = lax.rsqrt(jnp.mean(x_f32 * x_f32, axis=-1, keepdims=True) + RMS_EPS)
    return (x_f32 * inv_rms * gain_vec).astype(jnp.bfloat16)


def lora_proj(h_in, w_base, a_sel, b_sel):
    base_out = jnp.dot(h_in, w_base, preferred_element_type=jnp.float32)
    lora_mid = jnp.dot(h_in, a_sel, preferred_element_type=jnp.float32).astype(jnp.bfloat16)
    return base_out + (LORA_ALPHA / RANK) * jnp.dot(lora_mid, b_sel, preferred_element_type=jnp.float32)


def attend_head(head_item):
    q_head, k_head, v_head = head_item
    scores = jnp.dot(q_head, k_head.T, preferred_element_type=jnp.float32) * HEAD_DIM ** -0.5
    causal = jnp.arange(SEQ_LEN)[:, None] >= jnp.arange(SEQ_LEN)[None, :]
    prob_bf = jax.nn.softmax(jnp.where(causal, scores, -jnp.inf), axis=-1).astype(jnp.bfloat16)
    return jnp.dot(prob_bf, v_head, preferred_element_type=jnp.float32).astype(jnp.bfloat16)


def reference(x_in, adapter_ids, gain_attn, gain_mlp, w_q, w_k, w_v, w_o, w_gate, w_up, w_down,
              a_q, b_q, a_k, b_k, a_v, b_v, a_o, b_o, a_gate, b_gate, a_up, b_up, a_down, b_down):
    head_group = HEADS // KV_HEADS
    w_query = w_q.reshape(D_MODEL, Q_WIDTH)
    w_key = w_k.reshape(D_MODEL, KV_WIDTH)
    w_value = w_v.reshape(D_MODEL, KV_WIDTH)
    w_out = w_o.reshape(Q_WIDTH, D_MODEL)

    def one_sequence(seq_item):
        x_seq, adapter_id = seq_item
        h_norm = rms_scale(x_seq, gain_attn)
        q_all = lora_proj(h_norm, w_query, a_q[adapter_id], b_q[adapter_id].reshape(RANK, Q_WIDTH)).astype(jnp.bfloat16)
        k_all = lora_proj(h_norm, w_key, a_k[adapter_id], b_k[adapter_id].reshape(RANK, KV_WIDTH)).astype(jnp.bfloat16)
        v_all = lora_proj(h_norm, w_value, a_v[adapter_id], b_v[adapter_id].reshape(RANK, KV_WIDTH)).astype(jnp.bfloat16)
        q_heads = q_all.reshape(SEQ_LEN, HEADS, HEAD_DIM).transpose(1, 0, 2)
        k_heads = jnp.repeat(k_all.reshape(SEQ_LEN, KV_HEADS, HEAD_DIM).transpose(1, 0, 2), head_group, axis=0)
        v_heads = jnp.repeat(v_all.reshape(SEQ_LEN, KV_HEADS, HEAD_DIM).transpose(1, 0, 2), head_group, axis=0)
        att_heads = lax.map(attend_head, (q_heads, k_heads, v_heads))
        att_flat = att_heads.transpose(1, 0, 2).reshape(SEQ_LEN, Q_WIDTH)
        z_out = lora_proj(att_flat, w_out, a_o[adapter_id].reshape(Q_WIDTH, RANK), b_o[adapter_id])
        x_one = (x_seq.astype(jnp.float32) + z_out).astype(jnp.bfloat16)
        h_two = rms_scale(x_one, gain_mlp)
        z_gate = lora_proj(h_two, w_gate, a_gate[adapter_id], b_gate[adapter_id]).astype(jnp.bfloat16)
        z_up = lora_proj(h_two, w_up, a_up[adapter_id], b_up[adapter_id]).astype(jnp.bfloat16)
        mlp_mid = (jax.nn.silu(z_gate.astype(jnp.float32)) * z_up.astype(jnp.float32)).astype(jnp.bfloat16)
        z_down = lora_proj(mlp_mid, w_down, a_down[adapter_id], b_down[adapter_id])
        return (x_one.astype(jnp.float32) + z_down).astype(jnp.bfloat16)

    return lax.map(one_sequence, (x_in, adapter_ids))
```

```python
import functools

import jax
import jax.numpy as jnp
from jax import lax
from jax.experimental import pallas as pl
from jax.experimental.pallas import tpu as pltpu
from jax.sharding import PartitionSpec as P

value_a10 = 16
RMS_EPS = 1e-5
F32 = jnp.float32
BF16 = jnp.bfloat16
MESH = pl.DeviceIdType.MESH
ANY = pl.BlockSpec(memory_space=pl.ANY)
VMEM = pl.BlockSpec(memory_space=pltpu.VMEM)
VMEM_LIMIT = 67043328
LANES = 128
CHIPS = 4
LAG = 6


def rms_scale(x_in, gain_vec):
    x_f32 = x_in.astype(F32)
    inv_rms = lax.rsqrt(jnp.mean(x_f32 * x_f32, axis=-1, keepdims=True) + RMS_EPS)
    return (x_f32 * inv_rms * gain_vec).astype(BF16)


def causal_attention(q_flat, k_flat, v_flat, kv_heads, head_dim):
    num_seqs, seq_len = q_flat.shape[0], q_flat.shape[1]
    q_group = q_flat.reshape(num_seqs, seq_len, kv_heads, -1, head_dim)
    k_group = k_flat.reshape(num_seqs, seq_len, kv_heads, head_dim)
    v_group = v_flat.reshape(num_seqs, seq_len, kv_heads, head_dim)
    scores = jnp.einsum('bqngd,bknd->bngqk', q_group, k_group, preferred_element_type=F32) * head_dim ** -0.5
    causal = jnp.arange(seq_len)[:, None] >= jnp.arange(seq_len)[None, :]
    prob_bf = jax.nn.softmax(jnp.where(causal, scores, -jnp.inf), axis=-1).astype(BF16)
    att_out = jnp.einsum('bngqk,bknd->bqngd', prob_bf, v_group, preferred_element_type=F32)
    return att_out.astype(BF16).reshape(num_seqs, seq_len, -1)


class Exchange:
    def __init__(self, part, recv0, recv1, recv2, quart, done, out, sems):
        self.part, self.recv0, self.recv1, self.recv2 = part, recv0, recv1, recv2
        self.quart, self.done, self.out = quart, done, out
        (self.s0, self.r0, self.s1, self.r1, self.s2, self.r2, self.sa, self.ra, self.sb, self.rb, self.sc, self.rc,
         self.own) = sems
        me = lax.axis_index('tp')
        self.chip, self.core = me // 2, me % 2
        self.half = part.shape[0] // 2
        self.rows = self.half // CHIPS
        self.hrows = self.rows // 2
        self.right = self.device(self.chip + 1, self.core)
        self.left = self.device(self.chip + CHIPS - 1, self.core)
        self.partner = self.device(self.chip, 1 - self.core)

    def device(self, chip, core):
        return (chip % CHIPS) * 2 + core

    @staticmethod
    def scratch(seq_len, width, done_width):
        half = seq_len // 2
        rows = half // CHIPS
        dma = pltpu.SemaphoreType.DMA
        return [pltpu.VMEM((seq_len, width), BF16), pltpu.VMEM((2, half, width), BF16),
                pltpu.VMEM((2, 2, rows // 2, width), BF16), pltpu.VMEM((2, 2, rows, width), BF16),
                pltpu.VMEM((3, half, width), BF16), pltpu.VMEM((2, rows, done_width), BF16),
                dma((2,)), dma((2,)), dma((2, 2)), dma((2, 2)), dma((2, 2)), dma((2, 2)),
                dma((3, 2)), dma((3, 2)), dma((4, 2)), dma((4, 2)), dma((2,)), dma((2,)), dma((2,))]

    def barrier(self):
        sem = pltpu.get_barrier_semaphore()
        for other in (self.right, self.left, self.partner):
            pl.semaphore_signal(sem, inc=1, device_id={'tp': other}, device_id_type=MESH)
        pl.semaphore_wait(sem, 3)

    def send(self, src, dst, send_sem, recv_sem, other):
        return pltpu.make_async_remote_copy(src_ref=src, dst_ref=dst, send_sem=send_sem, recv_sem=recv_sem,
                                            device_id={'tp': other}, device_id_type=MESH)

    def slab(self, step):
        return pl.multiple_of(((self.chip + step) % CHIPS) * self.rows, self.rows)

    def own_row(self):
        return pl.multiple_of(self.core * self.half + self.slab(0), self.rows)

    def copy0(self, c):
        first = pl.multiple_of((1 - self.core) * self.half, self.half)
        return [self.send(self.part.at[pl.ds(first, self.half)], self.recv0.at[c % 2], self.s0.at[c % 2],
                          self.r0.at[c % 2], self.partner)]

    def copy1(self, c):
        quart, far = self.quart.at[c % 3], self.slab(2)
        low = pl.multiple_of(far + self.hrows, self.hrows)
        return [self.send(quart.at[pl.ds(far, self.hrows)], self.recv1.at[0, c % 2], self.s1.at[0, c % 2],
                          self.r1.at[0, c % 2], self.right),
                self.send(quart.at[pl.ds(low, self.hrows)], self.recv1.at[1, c % 2], self.s1.at[1, c % 2],
                          self.r1.at[1, c % 2], self.left)]

    def copy2(self, c):
        quart = self.quart.at[c % 3]
        return [self.send(quart.at[pl.ds(self.slab(1), self.rows)], self.recv2.at[0, c % 2], self.s2.at[0, c % 2],
                          self.r2.at[0, c % 2], self.right),
                self.send(quart.at[pl.ds(self.slab(CHIPS - 1), self.rows)], self.recv2.at[1, c % 2],
                          self.s2.at[1, c % 2], self.r2.at[1, c % 2], self.left)]

    def copy_a(self, c):
        dst = self.out.at[c, pl.ds(self.own_row(), self.rows)]
        return [self.send(self.done.at[c % 2], dst, self.sa.at[i, c % 2], self.ra.at[i, c % 2], other)
                for i, other in enumerate((self.right, self.left, self.partner))]

    def copy_own(self, c):
        return pltpu.make_async_copy(self.done.at[c % 2], self.out.at[c, pl.ds(self.own_row(), self.rows)],
                                     self.own.at[c % 2])

    def copy_b(self, c):
        base = self.core * self.half
        from_left = pl.multiple_of(base + self.slab(CHIPS - 1), self.rows)
        from_right = pl.multiple_of(base + self.slab(1), self.rows)
        low = pl.multiple_of(from_right + self.hrows, self.hrows)
        parts = ((from_left, self.hrows, self.right), (low, self.hrows, self.left),
                 (from_left, self.rows, self.partner), (from_right, self.rows, self.partner))
        return [self.send(self.out.at[c, pl.ds(first, size)], self.out.at[c, pl.ds(first, size)],
                          self.sb.at[i, c % 2], self.rb.at[i, c % 2], other)
                for i, (first, size, other) in enumerate(parts)]

    def copy_c(self, c):
        far = pl.multiple_of(self.core * self.half + self.slab(2), self.rows)
        rows = self.out.at[c, pl.ds(far, self.rows)]
        return [self.send(rows, rows, self.sc.at[c % 2], self.rc.at[c % 2], self.partner)]

    @staticmethod
    def start(copies):
        for copy in copies:
            copy.start()

    @staticmethod
    def wait_send(copies):
        for copy in copies:
            copy.wait_send()

    @staticmethod
    def wait_recv(copies):
        for copy in copies:
            copy.wait_recv()

    def add_pair(self, c):
        self.wait_recv(self.copy0(c))
        self.wait_send(self.copy0(c))
        quart, recv = self.quart.at[c % 3], self.recv0.at[c % 2]
        own = self.core * self.half

        @pl.loop(0, self.half // 16)
        def _(i):
            mine = self.part[pl.ds(pl.multiple_of(own + i * 16, 16), 16), :].astype(F32)
            rows = pl.ds(pl.multiple_of(i * 16, 16), 16)
            quart[rows, :] = (mine + recv[rows, :].astype(F32)).astype(BF16)

        self.start(self.copy1(c))

    def add_far(self, c):
        self.wait_recv(self.copy1(c))
        quart = self.quart.at[c % 3]
        for side, first in ((0, self.slab(1)), (1, self.slab(CHIPS - 1) + self.hrows)):
            rows = pl.ds(pl.multiple_of(first, self.hrows), self.hrows)
            quart[rows, :] = (quart[rows, :].astype(F32) + self.recv1[side, c % 2].astype(F32)).astype(BF16)
        self.start(self.copy2(c))

    def finish(self, c, finalize):
        self.wait_recv(self.copy2(c))
        self.wait_send(self.copy1(c))
        quart, slot = self.quart.at[c % 3], c % 2

        def total(first, size, columns):
            rows = pl.ds(pl.multiple_of(self.slab(0) + first, size), size)
            here = pl.ds(first, size)
            return (quart[rows, columns].astype(F32) + self.recv2[0, slot, here, columns].astype(F32)
                    + self.recv2[1, slot, here, columns].astype(F32))

        finalize(c, total, self.done.at[slot])
        self.start(self.copy_a(c))
        self.copy_own(c).start()

    def forward(self, c):
        self.wait_recv(self.copy_a(c))
        self.wait_send(self.copy2(c))
        self.start(self.copy_b(c))

    def cross(self, c):
        self.wait_recv(self.copy_b(c))
        self.wait_send(self.copy_a(c))
        self.copy_own(c).wait()
        self.start(self.copy_c(c))

    def close(self, c):
        self.wait_recv(self.copy_c(c))
        self.wait_send(self.copy_b(c))
        self.wait_send(self.copy_c(c))

    def stages(self, slot, count, compute, finalize, prefetch=None):
        def far(c):
            if prefetch is not None:
                prefetch(c)
            self.add_far(c)

        table = ((6, self.close), (5, self.cross), (4, self.forward),
                 (3, lambda c: self.finish(c, finalize)), (2, far), (1, self.add_pair))
        for lag, stage in table:
            @pl.when((slot >= lag) & (slot < count + lag))
            def _(lag=lag, stage=stage):
                stage(slot - lag)

        @pl.when(slot < count)
        def _():
            compute(slot)
            self.start(self.copy0(slot))


def lora_rows(mid, mask_row, b_ref, c, columns, rank):
    lane = lax.broadcasted_iota(jnp.int32, mid.shape, 1)
    mid = mid.astype(BF16).astype(F32)
    out = None
    for r in range(rank):
        keep = (mask_row > 0) & (lane % rank == r)
        column = jnp.sum(jnp.where(keep, mid, 0.0), axis=1, keepdims=True)
        term = column * b_ref[c, r:r + 1, columns].astype(F32)
        out = term if out is None else out + term
    return out


def out_kernel(count, scale, rank, att_ref, wo_ref, ao_ref, bo_ref, mask_ref, res_ref, gain_ref, h2_ref, x1_ref,
               *scratch):
    exchange = Exchange(*scratch[:6], h2_ref, scratch[6:19])
    exchange.barrier()
    width = wo_ref.shape[1]
    tile = 512

    def compute(c):
        att = att_ref[c]

        @pl.loop(0, width // tile)
        def _(n):
            columns = pl.ds(pl.multiple_of(n * tile, tile), tile)
            exchange.part[:, columns] = jnp.dot(att, wo_ref[:, columns], preferred_element_type=F32).astype(BF16)

        exchange.part[:, width:] = lax.dot_general(att, ao_ref[...], (((1,), (1,)), ((), ())),
                                                   preferred_element_type=F32).astype(BF16)

    def finalize(c, total, done):
        mask_row = mask_ref[pl.ds(c, 1), :]
        for first in range(0, exchange.rows, 16):
            here = pl.ds(first, 16)
            mid = total(first, 16, pl.ds(width, LANES))
            square = jnp.zeros((16, 1), F32)
            for n in range(width // tile):
                columns = pl.ds(n * tile, tile)
                lora = lora_rows(mid, mask_row, bo_ref, c, columns, rank)
                x_one = (res_ref[c, here, columns].astype(F32) + (total(first, 16, columns) + scale * lora)).astype(BF16)
                x1_ref[c, here, columns] = x_one
                x_one = x_one.astype(F32)
                square += jnp.sum(x_one * x_one, axis=1, keepdims=True)
            inv_rms = lax.rsqrt(square / width + RMS_EPS)
            for n in range(width // tile):
                columns = pl.ds(n * tile, tile)
                x_one = x1_ref[c, here, columns].astype(F32)
                done[here, columns] = (x_one * inv_rms * gain_ref[:, columns]).astype(BF16)

    @pl.loop(0, count + LAG)
    def _(slot):
        exchange.stages(slot, count, compute, finalize)


def mlp_kernel(count, scale, rank, h2_ref, wg_ref, wu_ref, wd_ref, agu_ref, bg_ref, bu_ref, gmask_ref, ad_ref, bd_ref,
               mask_ref, res_ref, y_ref, *scratch):
    exchange = Exchange(*scratch[:6], y_ref, scratch[6:19])
    wg, wu, wd, hbuf, mid_buf, t_buf, rbuf, sem_g, sem_u, sem_d, sem_h, sem_r = scratch[19:]
    gtile, dtile = wg.shape[2], wd.shape[2]
    width = wd_ref.shape[1]

    def load_h(c):
        return pltpu.make_async_copy(h2_ref.at[c], hbuf, sem_h)

    def load_r(c):
        return pltpu.make_async_copy(res_ref.at[c], rbuf.at[c % 2], sem_r.at[c % 2])

    def load_g(j):
        columns = pl.ds(pl.multiple_of(j * gtile, gtile), gtile)
        return (pltpu.make_async_copy(wg_ref.at[:, columns], wg.at[j], sem_g.at[j]),
                pltpu.make_async_copy(wu_ref.at[:, columns], wu.at[j], sem_u.at[j]))

    def load_d(n):
        columns = pl.ds(pl.multiple_of(n * dtile, dtile), dtile)
        return pltpu.make_async_copy(wd_ref.at[:, columns], wd.at[n], sem_d.at[n])

    load_h(0).start()
    for j in range(wg.shape[0]):
        for copy in load_g(j):
            copy.start()
    for n in range(wd.shape[0]):
        load_d(n).start()
    exchange.barrier()

    def compute(c):
        load_h(c).wait()
        t_all = lax.dot_general(hbuf[...], agu_ref[...], (((1,), (1,)), ((), ())), preferred_element_type=F32)
        t_buf[...] = jnp.where(gmask_ref[pl.ds(c, 1), :] > 0, t_all.astype(BF16).astype(F32), 0.0).astype(BF16)

        @pl.loop(0, wg.shape[0])
        def _(j):
            @pl.when(c == 0)
            def _():
                for copy in load_g(j):
                    copy.wait()
            columns = pl.ds(pl.multiple_of(j * gtile, gtile), gtile)
            gate = jnp.dot(hbuf[...], wg[j], preferred_element_type=F32)
            gate += scale * jnp.dot(t_buf[...], bg_ref[:, columns], preferred_element_type=F32)
            gate = gate.astype(BF16).astype(F32)
            up = jnp.dot(hbuf[...], wu[j], preferred_element_type=F32)
            up += scale * jnp.dot(t_buf[...], bu_ref[:, columns], preferred_element_type=F32)
            up = up.astype(BF16).astype(F32)
            mid_buf[:, columns] = (jax.nn.silu(gate) * up).astype(BF16)

        @pl.when(c + 1 < count)
        def _():
            load_h(c + 1).start()

        @pl.loop(0, wd.shape[0])
        def _(n):
            @pl.when(c == 0)
            def _():
                load_d(n).wait()
            columns = pl.ds(pl.multiple_of(n * dtile, dtile), dtile)
            exchange.part[:, columns] = jnp.dot(mid_buf[...], wd[n], preferred_element_type=F32).astype(BF16)

        exchange.part[:, width:] = lax.dot_general(mid_buf[...], ad_ref[...], (((1,), (1,)), ((), ())),
                                                   preferred_element_type=F32).astype(BF16)

    def finalize(c, total, done):
        load_r(c).wait()
        mask_row = mask_ref[pl.ds(c, 1), :]
        for first in range(0, exchange.rows, 16):
            here = pl.ds(first, 16)
            mid = total(first, 16, pl.ds(width, LANES))
            for n in range(width // 512):
                columns = pl.ds(n * 512, 512)
                lora = lora_rows(mid, mask_row, bd_ref, c, columns, rank)
                res = rbuf[c % 2, here, columns].astype(F32)
                done[here, columns] = (res + (total(first, 16, columns) + scale * lora)).astype(BF16)

    @pl.loop(0, count + LAG)
    def _(slot):
        exchange.stages(slot, count, compute, finalize, lambda c: load_r(c).start())


def solution(mesh):
    act_spec = P('dp', None, None)
    w_head_spec = P(None, 'tp', None)
    w_out_spec = P('tp', None, None)
    w_col_spec = P(None, 'tp')
    w_row_spec = P('tp', None)
    a_rank_spec = P(None, None, 'tp')
    b_head_spec = P(None, None, 'tp', None)
    b_col_spec = P(None, None, 'tp')
    a_head_spec = P(None, 'tp', None, None)
    a_row_spec = P(None, 'tp', None)
    in_specs = (act_spec, P('dp'), P(None), P(None), w_head_spec, w_head_spec, w_head_spec, w_out_spec,
                w_col_spec, w_col_spec, w_row_spec, a_rank_spec, b_head_spec, a_rank_spec, b_head_spec,
                a_rank_spec, b_head_spec, a_head_spec, b_col_spec, a_rank_spec, b_col_spec,
                a_rank_spec, b_col_spec, a_row_spec, b_col_spec)

    def local_layer(x_in, adapter_ids, gain_attn, gain_mlp, w_q, w_k, w_v, w_o, w_gate, w_up, w_down,
                    a_q, b_q, a_k, b_k, a_v, b_v, a_o, b_o, a_gate, b_gate, a_up, b_up, a_down, b_down):
        count, seq_len, width = x_in.shape
        adapters, rank = b_q.shape[:2]
        mixed = adapters * rank
        scale = value_a10 / rank
        ff = w_gate.shape[1]

        a_loc = jnp.stack([a.transpose(2, 0, 1) for a in (a_q, a_k, a_v, a_gate, a_up)], 1)
        cols = b_o.shape[2]
        packed = jnp.concatenate([a_loc.reshape(-1, cols), b_o.reshape(-1, cols), b_down.reshape(-1, cols)], 0)
        packed = lax.all_gather(packed, 'tp', axis=0)
        n_a = a_loc.size // cols
        a_all = packed[:, :n_a].reshape(-1, 5, adapters, width).transpose(1, 0, 2, 3).reshape(5, mixed, width)
        b_rows = packed[:, n_a:].reshape(-1, 2, adapters, rank, cols).transpose(1, 2, 3, 0, 4)
        b_rows = jnp.take(b_rows.reshape(2, adapters, rank, width), adapter_ids, axis=1)

        rank_major = jnp.arange(mixed) % adapters == adapter_ids[:, None]
        id_major = jnp.arange(mixed) // rank == adapter_ids[:, None]
        mask_row = jnp.pad(id_major, ((0, 0), (0, LANES - mixed))).astype(F32)
        mask_two = jnp.tile(rank_major, (1, 2)).astype(F32)

        h_norm = rms_scale(x_in, gain_attn)
        w_all = jnp.concatenate([w.reshape(width, -1) for w in (w_q, w_k, w_v)], 1)
        base = jnp.einsum('bsd,de->bse', h_norm, w_all, preferred_element_type=F32)
        mids = jnp.einsum('bsd,rd->bsr', h_norm, a_all[:3].reshape(-1, width), preferred_element_type=F32).astype(BF16)
        mids = jnp.where(jnp.tile(rank_major, (1, 3))[:, None], mids, jnp.zeros((), BF16))
        n_q, n_k = w_q[0].size, w_k[0].size
        b_all = [b.transpose(1, 0, 2, 3).reshape(mixed, -1) for b in (b_q, b_k, b_v)]
        b_all = jnp.concatenate([jnp.pad(b, ((0, 0), (first, w_all.shape[1] - first - b.shape[1])))
                                 for b, first in zip(b_all, (0, n_q, n_q + n_k))], 0)
        qkv = (base + scale * jnp.einsum('bsr,re->bse', mids, b_all, preferred_element_type=F32)).astype(BF16)
        att = causal_attention(qkv[..., :n_q], qkv[..., n_q:n_q + n_k], qkv[..., n_q + n_k:], w_k.shape[1],
                               w_k.shape[2])

        me = lax.axis_index('tp')
        own = seq_len // 2 // CHIPS
        own_row = (me % 2) * (seq_len // 2) + (me // 2) * own
        res = lax.dynamic_slice_in_dim(x_in, own_row, own, axis=1)
        a_o_t = jnp.pad(a_o.transpose(0, 3, 1, 2).reshape(mixed, -1), ((0, LANES - mixed), (0, 0)))
        exchange_scratch = Exchange.scratch(seq_len, width + LANES, width)
        h_two, x_one = pl.pallas_call(
            functools.partial(out_kernel, count, scale, rank),
            out_shape=(jax.ShapeDtypeStruct(x_in.shape, BF16), jax.ShapeDtypeStruct(res.shape, BF16)),
            in_specs=[VMEM] * 7, out_specs=(ANY, VMEM), scratch_shapes=exchange_scratch,
            compiler_params=pltpu.CompilerParams(collective_id=0, has_side_effects=True, vmem_limit_bytes=VMEM_LIMIT),
        )(att, w_o.reshape(-1, width), a_o_t, b_rows[0], mask_row, res, gain_mlp.reshape(1, -1))

        b_cols = [b.transpose(1, 0, 2).reshape(mixed, -1) for b in (b_gate, b_up)]
        b_g = jnp.pad(b_cols[0], ((0, mixed), (0, 0)))
        b_u = jnp.pad(b_cols[1], ((mixed, 0), (0, 0)))
        a_d_t = jnp.pad(a_down.transpose(0, 2, 1).reshape(mixed, -1), ((0, LANES - mixed), (0, 0)))
        gtile, dtile = 256, 512
        dma = pltpu.SemaphoreType.DMA
        return pl.pallas_call(
            functools.partial(mlp_kernel, count, scale, rank),
            out_shape=jax.ShapeDtypeStruct(x_in.shape, BF16),
            in_specs=[ANY] * 4 + [VMEM] * 7 + [ANY], out_specs=ANY,
            scratch_shapes=exchange_scratch + [
                pltpu.VMEM((ff // gtile, width, gtile), BF16), pltpu.VMEM((ff // gtile, width, gtile), BF16),
                pltpu.VMEM((width // dtile, ff, dtile), BF16), pltpu.VMEM((seq_len, width), BF16),
                pltpu.VMEM((seq_len, ff), BF16), pltpu.VMEM((seq_len, 2 * mixed), BF16),
                pltpu.VMEM((2, own, width), BF16), dma((ff // gtile,)), dma((ff // gtile,)), dma((width // dtile,)),
                dma, dma((2,))],
            compiler_params=pltpu.CompilerParams(collective_id=1, has_side_effects=True, vmem_limit_bytes=VMEM_LIMIT),
        )(h_two, w_gate, w_up, w_down, a_all[3:].reshape(2 * mixed, width), b_g, b_u, mask_two, a_d_t, b_rows[1],
          mask_row, x_one)

    return jax.shard_map(local_layer, mesh=mesh, in_specs=in_specs, out_specs=act_spec, check_vma=False)
```

```python
import functools

import jax
import jax.numpy as jnp
from jax import lax
from jax.experimental import pallas as pl
from jax.experimental.pallas import tpu as pltpu
from jax.sharding import PartitionSpec as P

value_a10 = 16
RMS_EPS = 1e-5
F32 = jnp.float32
BF16 = jnp.bfloat16
MESH = pl.DeviceIdType.MESH
ANY = pl.BlockSpec(memory_space=pl.ANY)
VMEM = pl.BlockSpec(memory_space=pltpu.VMEM)
VMEM_LIMIT = 67043328
LANES = 128
CHIPS = 4
LAG = 6


class Exchange:
    def __init__(self, part, recv0, recv1, recv2, quart, done, out, sems):
        self.part, self.recv0, self.recv1, self.recv2 = part, recv0, recv1, recv2
        self.quart, self.done, self.out = quart, done, out
        (self.s0, self.r0, self.s1, self.r1, self.s2, self.r2, self.sa, self.ra, self.sb, self.rb, self.sc, self.rc,
         self.own) = sems
        me = lax.axis_index('tp')
        self.chip, self.core = me // 2, me % 2
        self.half = part.shape[0] // 2
        self.rows = self.half // CHIPS
        self.hrows = self.rows // 2
        self.right = self.device(self.chip + 1, self.core)
        self.left = self.device(self.chip + CHIPS - 1, self.core)
        self.partner = self.device(self.chip, 1 - self.core)

    def device(self, chip, core):
        return (chip % CHIPS) * 2 + core

    @staticmethod
    def scratch(seq_len, width, done_width):
        half = seq_len // 2
        rows = half // CHIPS
        dma = pltpu.SemaphoreType.DMA
        return [pltpu.VMEM((seq_len, width), BF16), pltpu.VMEM((2, half, width), BF16),
                pltpu.VMEM((2, 2, rows // 2, width), BF16), pltpu.VMEM((2, 2, rows, width), BF16),
                pltpu.VMEM((3, half, width), BF16), pltpu.VMEM((2, rows, done_width), BF16),
                dma((2,)), dma((2,)), dma((2, 2)), dma((2, 2)), dma((2, 2)), dma((2, 2)),
                dma((3, 2)), dma((3, 2)), dma((4, 2)), dma((4, 2)), dma((2,)), dma((2,)), dma((2,))]

    def barrier(self):
        sem = pltpu.get_barrier_semaphore()
        for other in (self.right, self.left, self.partner):
            pl.semaphore_signal(sem, inc=1, device_id={'tp': other}, device_id_type=MESH)
        pl.semaphore_wait(sem, 3)

    def send(self, src, dst, send_sem, recv_sem, other):
        return pltpu.make_async_remote_copy(src_ref=src, dst_ref=dst, send_sem=send_sem, recv_sem=recv_sem,
                                            device_id={'tp': other}, device_id_type=MESH)

    def slab(self, step):
        return pl.multiple_of(((self.chip + step) % CHIPS) * self.rows, self.rows)

    def own_row(self):
        return pl.multiple_of(self.core * self.half + self.slab(0), self.rows)

    def copy0(self, c):
        first = pl.multiple_of((1 - self.core) * self.half, self.half)
        return [self.send(self.part.at[pl.ds(first, self.half)], self.recv0.at[c % 2], self.s0.at[c % 2],
                          self.r0.at[c % 2], self.partner)]

    def copy1(self, c):
        quart, far = self.quart.at[c % 3], self.slab(2)
        low = pl.multiple_of(far + self.hrows, self.hrows)
        return [self.send(quart.at[pl.ds(far, self.hrows)], self.recv1.at[0, c % 2], self.s1.at[0, c % 2],
                          self.r1.at[0, c % 2], self.right),
                self.send(quart.at[pl.ds(low, self.hrows)], self.recv1.at[1, c % 2], self.s1.at[1, c % 2],
                          self.r1.at[1, c % 2], self.left)]

    def copy2(self, c):
        quart = self.quart.at[c % 3]
        return [self.send(quart.at[pl.ds(self.slab(1), self.rows)], self.recv2.at[0, c % 2], self.s2.at[0, c % 2],
                          self.r2.at[0, c % 2], self.right),
                self.send(quart.at[pl.ds(self.slab(CHIPS - 1), self.rows)], self.recv2.at[1, c % 2],
                          self.s2.at[1, c % 2], self.r2.at[1, c % 2], self.left)]

    def copy_a(self, c):
        dst = self.out.at[c, pl.ds(self.own_row(), self.rows)]
        return [self.send(self.done.at[c % 2], dst, self.sa.at[i, c % 2], self.ra.at[i, c % 2], other)
                for i, other in enumerate((self.right, self.left, self.partner))]

    def copy_own(self, c):
        return pltpu.make_async_copy(self.done.at[c % 2], self.out.at[c, pl.ds(self.own_row(), self.rows)],
                                     self.own.at[c % 2])

    def copy_b(self, c):
        base = self.core * self.half
        from_left = pl.multiple_of(base + self.slab(CHIPS - 1), self.rows)
        from_right = pl.multiple_of(base + self.slab(1), self.rows)
        low = pl.multiple_of(from_right + self.hrows, self.hrows)
        parts = ((from_left, self.hrows, self.right), (low, self.hrows, self.left),
                 (from_left, self.rows, self.partner), (from_right, self.rows, self.partner))
        return [self.send(self.out.at[c, pl.ds(first, size)], self.out.at[c, pl.ds(first, size)],
                          self.sb.at[i, c % 2], self.rb.at[i, c % 2], other)
                for i, (first, size, other) in enumerate(parts)]

    def copy_c(self, c):
        far = pl.multiple_of(self.core * self.half + self.slab(2), self.rows)
        rows = self.out.at[c, pl.ds(far, self.rows)]
        return [self.send(rows, rows, self.sc.at[c % 2], self.rc.at[c % 2], self.partner)]

    @staticmethod
    def start(copies):
        for copy in copies:
            copy.start()

    @staticmethod
    def wait_send(copies):
        for copy in copies:
            copy.wait_send()

    @staticmethod
    def wait_recv(copies):
        for copy in copies:
            copy.wait_recv()

    def add_pair(self, c):
        self.wait_recv(self.copy0(c))
        self.wait_send(self.copy0(c))
        quart, recv = self.quart.at[c % 3], self.recv0.at[c % 2]
        own = self.core * self.half

        @pl.loop(0, self.half // 16)
        def _(i):
            mine = self.part[pl.ds(pl.multiple_of(own + i * 16, 16), 16), :].astype(F32)
            rows = pl.ds(pl.multiple_of(i * 16, 16), 16)
            quart[rows, :] = (mine + recv[rows, :].astype(F32)).astype(BF16)

        self.start(self.copy1(c))

    def add_far(self, c):
        self.wait_recv(self.copy1(c))
        quart = self.quart.at[c % 3]
        for side, first in ((0, self.slab(1)), (1, self.slab(CHIPS - 1) + self.hrows)):
            rows = pl.ds(pl.multiple_of(first, self.hrows), self.hrows)
            quart[rows, :] = (quart[rows, :].astype(F32) + self.recv1[side, c % 2].astype(F32)).astype(BF16)
        self.start(self.copy2(c))

    def finish(self, c, finalize):
        self.wait_recv(self.copy2(c))
        self.wait_send(self.copy1(c))
        quart, slot = self.quart.at[c % 3], c % 2

        def total(first, size, columns):
            rows = pl.ds(pl.multiple_of(self.slab(0) + first, size), size)
            here = pl.ds(first, size)
            return (quart[rows, columns].astype(F32) + self.recv2[0, slot, here, columns].astype(F32)
                    + self.recv2[1, slot, here, columns].astype(F32))

        finalize(c, total, self.done.at[slot])
        self.start(self.copy_a(c))
        self.copy_own(c).start()

    def forward(self, c):
        self.wait_recv(self.copy_a(c))
        self.wait_send(self.copy2(c))
        self.start(self.copy_b(c))

    def cross(self, c):
        self.wait_recv(self.copy_b(c))
        self.wait_send(self.copy_a(c))
        self.copy_own(c).wait()
        self.start(self.copy_c(c))

    def close(self, c):
        self.wait_recv(self.copy_c(c))
        self.wait_send(self.copy_b(c))
        self.wait_send(self.copy_c(c))

    def stages(self, slot, count, finalize, prefetch):
        def far(c):
            prefetch(c)
            self.add_far(c)

        table = ((6, self.close), (5, self.cross), (4, self.forward),
                 (3, lambda c: self.finish(c, finalize)), (2, far), (1, self.add_pair))
        for lag, stage in table:
            @pl.when((slot >= lag) & (slot < count + lag))
            def _(lag=lag, stage=stage):
                stage(slot - lag)


class Gather:
    def __init__(self, exchange, own, full, sems):
        self.ex, self.own, self.full = exchange, own, full
        self.sa, self.ra, self.sb, self.rb, self.sc, self.rc = sems
        self.rows = own.shape[1]
        self.half = self.rows // 2

    @staticmethod
    def scratch():
        dma = pltpu.SemaphoreType.DMA
        return [dma((2, 3)), dma((2, 3)), dma((2, 4)), dma((2, 4)), dma((2,)), dma((2,))]

    def first(self, device):
        return pl.multiple_of(device * self.rows, self.rows)

    def copy_a(self, p):
        ex = self.ex
        dst = self.full.at[p, pl.ds(self.first(ex.device(ex.chip, ex.core)), self.rows)]
        return [ex.send(self.own.at[p], dst, self.sa.at[p, i], self.ra.at[p, i], other)
                for i, other in enumerate((ex.right, ex.left, ex.partner))]

    def copy_b(self, p):
        ex = self.ex
        from_left, from_right = self.first(ex.left), self.first(ex.right)
        low = pl.multiple_of(from_right + self.half, self.half)
        parts = ((from_left, self.half, ex.right), (low, self.half, ex.left),
                 (from_left, self.rows, ex.partner), (from_right, self.rows, ex.partner))
        return [ex.send(self.full.at[p, pl.ds(first, size)], self.full.at[p, pl.ds(first, size)], self.sb.at[p, i],
                        self.rb.at[p, i], other) for i, (first, size, other) in enumerate(parts)]

    def copy_c(self, p):
        ex = self.ex
        rows = self.full.at[p, pl.ds(self.first(ex.device(ex.chip + 2, ex.core)), self.rows)]
        return [ex.send(rows, rows, self.sc.at[p], self.rc.at[p], ex.partner)]

    def begin(self, p):
        me = self.ex.device(self.ex.chip, self.ex.core)
        self.ex.start(self.copy_a(p))
        self.full[p, pl.ds(self.first(me), self.rows), :] = self.own[p]

    def forward(self, p):
        self.ex.wait_recv(self.copy_a(p))
        self.ex.start(self.copy_b(p))

    def cross(self, p):
        self.ex.wait_recv(self.copy_b(p))
        self.ex.start(self.copy_c(p))

    def close(self, p):
        self.ex.wait_recv(self.copy_c(p))
        for copies in (self.copy_a, self.copy_b, self.copy_c):
            self.ex.wait_send(copies(p))


def dot_t(a, b):
    return lax.dot_general(a, b, (((1,), (1,)), ((), ())), preferred_element_type=F32)


def dot(a, b):
    return jnp.dot(a, b, preferred_element_type=F32)


def layer_kernel(count, scale, rank, heads, head_dim, x_ref, wqkv_ref, wo_ref, wg_ref, wu_ref, wd_ref, own_ref,
                 bqkv_ref, bg_ref, bu_ref, ao_ref, ad_ref, masks_ref, amask_ref, gain_a_ref, gain_m_ref, y_ref, h2_ref,
                 *scratch):
    one = Exchange(*scratch[:6], h2_ref, scratch[6:19])
    two = Exchange(*scratch[19:25], y_ref, scratch[25:38])
    full = scratch[38]
    gather = Gather(one, own_ref, full, scratch[39:45])
    (wqkv, wo, wd, ring, ubuf, qkv, att, mid, t_buf, x1, rbuf, sem_w, sem_d, sem_ring, sem_x, sem_h, sem_r) = scratch[45:]
    seq_len, width = ubuf.shape
    gtile, dtile = ring.shape[2], wd.shape[2]
    pairs, downs = mid.shape[1] // gtile, wd.shape[0]
    mixed = full.shape[1]

    def load_x(c):
        return pltpu.make_async_copy(x_ref.at[c], ubuf, sem_x)

    def load_h(c):
        return pltpu.make_async_copy(h2_ref.at[c], ubuf, sem_h)

    def load_r(c):
        return pltpu.make_async_copy(x_ref.at[c, pl.ds(one.own_row(), one.rows)], rbuf.at[c % 2], sem_r.at[c % 2])

    def load_d(n):
        columns = pl.ds(pl.multiple_of(n * dtile, dtile), dtile)
        return pltpu.make_async_copy(wd_ref.at[:, columns], wd.at[n], sem_d.at[n])

    def load_tile(w_ref, c, j, side):
        place = ((c * pairs + j) * 2 + side) % 3
        columns = pl.ds(pl.multiple_of(j * gtile, gtile), gtile)
        return pltpu.make_async_copy(w_ref.at[:, columns], ring.at[place], sem_ring.at[place]), place

    load_qkv = pltpu.make_async_copy(wqkv_ref, wqkv, sem_w.at[0])
    load_o = pltpu.make_async_copy(wo_ref, wo, sem_w.at[1])

    load_x(0).start()
    load_qkv.start()
    load_o.start()
    one.barrier()
    gather.begin(0)
    gather.begin(1)
    for w_ref, j, side in ((wg_ref, 0, 0), (wu_ref, 0, 1), (wg_ref, 1, 0)):
        load_tile(w_ref, 0, j, side)[0].start()
    for n in range(downs):
        load_d(n).start()

    def attention(c):
        load_x(c).wait()

        @pl.loop(0, seq_len // 16)
        def _(i):
            rows = pl.ds(pl.multiple_of(i * 16, 16), 16)
            value = ubuf[rows, :].astype(F32)
            inv_rms = lax.rsqrt(jnp.sum(value * value, axis=1, keepdims=True) / width + RMS_EPS)
            ubuf[rows, :] = (value * inv_rms * gain_a_ref[...]).astype(BF16)

        @pl.when(c == 0)
        def _():
            gather.forward(0)
            gather.cross(0)
            load_qkv.wait()
            load_o.wait()
            gather.close(0)

        @pl.when(c == 1)
        def _():
            gather.forward(1)

        @pl.when(c == 2)
        def _():
            gather.cross(1)

        keep = masks_ref[c, :, 0:mixed] > 0
        t_buf[...] = jnp.where(keep, dot_t(ubuf[...], full[0]).astype(BF16).astype(F32), 0.0).astype(BF16)

        @pl.loop(0, qkv.shape[1] // 256)
        def _(n):
            columns = pl.ds(pl.multiple_of(n * 256, 256), 256)
            base = dot(ubuf[...], wqkv[:, columns])
            qkv[:, columns] = (base + scale * dot(t_buf[...], bqkv_ref[:, columns])).astype(BF16)

        @pl.when((c + 1 < count) & (c < LAG))
        def _():
            load_x(c + 1).start()

        kv_heads = (qkv.shape[1] // head_dim - heads) // 2
        causal = (lax.broadcasted_iota(jnp.int32, (seq_len, seq_len), 0)
                  >= lax.broadcasted_iota(jnp.int32, (seq_len, seq_len), 1))
        for j in range(heads):
            kv = heads + j * kv_heads // heads
            query, key, value = (qkv[:, i * head_dim:(i + 1) * head_dim] for i in (j, kv, kv + kv_heads))
            scores = jnp.where(causal, dot_t(query, key) * head_dim ** -0.5, -jnp.inf)
            prob = jnp.exp(scores - jnp.max(scores, axis=1, keepdims=True))
            prob = (prob / jnp.sum(prob, axis=1, keepdims=True)).astype(BF16)
            att[:, j * head_dim:(j + 1) * head_dim] = dot(prob, value).astype(BF16)

        @pl.loop(0, width // 512)
        def _(n):
            columns = pl.ds(pl.multiple_of(n * 512, 512), 512)
            one.part[:, columns] = dot(att[...], wo[:, columns]).astype(BF16)

        pad = jnp.zeros((seq_len, LANES - ao_ref.shape[0]), F32)
        one.part[:, width:] = jnp.concatenate([dot_t(att[...], ao_ref[...]), pad], 1).astype(BF16)

        @pl.when(c == 2)
        def _():
            gather.close(1)

    def mlp(c):
        load_h(c).wait()
        keep = masks_ref[c, :, mixed:2 * mixed] > 0
        t_buf[...] = jnp.where(keep, dot_t(ubuf[...], full[1]).astype(BF16).astype(F32), 0.0).astype(BF16)

        def product(w_ref, b_ref, j, side):
            copy, place = load_tile(w_ref, c, j, side)
            copy.wait()
            columns = pl.ds(pl.multiple_of(j * gtile, gtile), gtile)
            out = dot(ubuf[...], ring[place]) + scale * dot(t_buf[...], b_ref[:, columns])
            return out.astype(BF16)

        def refill(w_ref, j, side):
            wrap = j // pairs
            @pl.when(c + wrap < count)
            def _():
                load_tile(w_ref, c + wrap, j % pairs, side)[0].start()

        @pl.loop(0, pairs)
        def _(j):
            columns = pl.ds(pl.multiple_of(j * gtile, gtile), gtile)
            mid[:, columns] = product(wg_ref, bg_ref, j, 0)
            refill(wu_ref, j + 1, 1)
            up = product(wu_ref, bu_ref, j, 1)
            refill(wg_ref, j + 2, 0)
            mid[:, columns] = (jax.nn.silu(mid[:, columns].astype(F32)) * up.astype(F32)).astype(BF16)

        @pl.when(c + LAG + 1 < count)
        def _():
            load_x(c + LAG + 1).start()

        @pl.loop(0, downs)
        def _(n):
            @pl.when(c == 0)
            def _():
                load_d(n).wait()
            columns = pl.ds(pl.multiple_of(n * dtile, dtile), dtile)
            two.part[:, columns] = dot(mid[...], wd[n]).astype(BF16)

        pad = jnp.zeros((seq_len, LANES - ad_ref.shape[0]), F32)
        two.part[:, width:] = jnp.concatenate([dot_t(mid[...], ad_ref[...]), pad], 1).astype(BF16)

    def totals(c, total, exchange, first_b):
        tile = width // (mixed // own_ref.shape[1])
        lanes = total(0, exchange.rows, pl.ds(width, LANES)).astype(BF16).astype(F32)
        lane = lax.broadcasted_iota(jnp.int32, lanes.shape, 1)
        keep = masks_ref[c, :, 2 * mixed:2 * mixed + LANES] > 0
        lanes = jnp.where(keep, lanes, 0.0)
        columns = [jnp.sum(jnp.where(lane % rank == r, lanes, 0.0), axis=1, keepdims=True) for r in range(rank)]
        chosen = amask_ref[c] > 0
        for n in range(width // tile):
            lora = None
            for r in range(rank):
                b_all = full[1, n * own_ref.shape[1] + first_b:n * own_ref.shape[1] + first_b + 8,
                             r * tile:(r + 1) * tile].astype(F32)
                b_row = jnp.sum(jnp.where(chosen[:, :1], b_all, 0.0), axis=0, keepdims=True)
                lora = columns[r] * b_row if lora is None else lora + columns[r] * b_row
            yield pl.ds(n * tile, tile), total(0, exchange.rows, pl.ds(n * tile, tile)) + scale * lora

    def finish_one(c, total, done):
        load_r(c).wait()
        square = jnp.zeros((one.rows, 1), F32)
        for columns, z_out in totals(c, total, one, 16):
            x_one = (rbuf[c % 2, :, columns].astype(F32) + z_out).astype(BF16)
            x1[c, :, columns] = x_one
            x_one = x_one.astype(F32)
            square += jnp.sum(x_one * x_one, axis=1, keepdims=True)
        inv_rms = lax.rsqrt(square / width + RMS_EPS)
        for n in range(width // 512):
            columns = pl.ds(n * 512, 512)
            done[:, columns] = (x1[c, :, columns].astype(F32) * inv_rms * gain_m_ref[:, columns]).astype(BF16)

    def finish_two(c, total, done):
        for columns, z_out in totals(c, total, two, 24):
            done[:, columns] = (x1[c, :, columns].astype(F32) + z_out).astype(BF16)

    @pl.loop(0, count + 2 * LAG)
    def _(slot):
        one.stages(slot, count, finish_one, lambda c: load_r(c).start())

        @pl.when(slot < count)
        def _():
            attention(slot)
            one.start(one.copy0(slot))

        @pl.when((slot >= LAG) & (slot < count + LAG))
        def _():
            load_h(slot - LAG).start()

        two.stages(slot - LAG, count, finish_two, lambda c: None)

        @pl.when((slot >= LAG) & (slot < count + LAG))
        def _():
            mlp(slot - LAG)
            two.start(two.copy0(slot - LAG))


def solution(mesh):
    act_spec = P('dp', None, None)
    w_head_spec = P(None, 'tp', None)
    w_out_spec = P('tp', None, None)
    w_col_spec = P(None, 'tp')
    w_row_spec = P('tp', None)
    a_rank_spec = P(None, None, 'tp')
    b_head_spec = P(None, None, 'tp', None)
    b_col_spec = P(None, None, 'tp')
    a_head_spec = P(None, 'tp', None, None)
    a_row_spec = P(None, 'tp', None)
    in_specs = (act_spec, P('dp'), P(None), P(None), w_head_spec, w_head_spec, w_head_spec, w_out_spec,
                w_col_spec, w_col_spec, w_row_spec, a_rank_spec, b_head_spec, a_rank_spec, b_head_spec,
                a_rank_spec, b_head_spec, a_head_spec, b_col_spec, a_rank_spec, b_col_spec,
                a_rank_spec, b_col_spec, a_row_spec, b_col_spec)

    def local_layer(x_in, adapter_ids, gain_attn, gain_mlp, w_q, w_k, w_v, w_o, w_gate, w_up, w_down,
                    a_q, b_q, a_k, b_k, a_v, b_v, a_o, b_o, a_gate, b_gate, a_up, b_up, a_down, b_down):
        count, seq_len, width = x_in.shape
        adapters, rank = b_q.shape[:2]
        mixed = adapters * rank
        scale = value_a10 / rank
        ff = w_gate.shape[1]

        group = mesh.shape['tp']
        head_dim = w_k.shape[2]
        n_q, n_k = w_q[0].size, w_k[0].size

        def plane(b):
            return b.transpose(1, 0, 2).reshape(group, adapters, -1)

        def planes(parts):
            zero = jnp.zeros_like(parts[0])
            return jnp.stack(list(parts) + [zero] * (4 - len(parts)), 1).reshape(4 * mixed, -1)

        a_loc = [a.transpose(2, 0, 1).reshape(adapters, width) for a in (a_q, a_k, a_v, a_gate, a_up)]
        b_loc = [b.reshape(adapters, -1) for b in (b_o, b_down)]
        own = jnp.stack([jnp.concatenate(a_loc[:3] + [jnp.zeros_like(a_loc[0])], 0),
                         jnp.concatenate(a_loc[3:] + b_loc, 0)])
        b_in = [plane(b.reshape(adapters, rank, -1)) for b in (b_q, b_k, b_v)]
        n_all = n_q + 2 * n_k
        b_qkv = planes([jnp.pad(b, ((0, 0), (0, 0), (at, n_all - at - b.shape[2])))
                        for b, at in zip(b_in, (0, n_q, n_q + n_k))])
        b_g = planes([plane(b_gate)])
        b_u = planes([jnp.zeros_like(plane(b_up)), plane(b_up)])

        index = jnp.arange(4 * mixed)
        mine = index % adapters == adapter_ids[:, None]
        index_plane = index // adapters % 4
        lane = jnp.arange(LANES)
        masks = jnp.concatenate([mine & (index_plane < 3), mine & (index_plane < 2),
                                 lane // rank == adapter_ids[:, None]], 1).astype(F32)
        amask = jnp.broadcast_to((jnp.arange(adapters) == adapter_ids[:, None])[:, :, None].astype(F32),
                                 (count, adapters, LANES))
        w_all = jnp.concatenate([w.reshape(width, -1) for w in (w_q, w_k, w_v)], 1)
        a_o_t = a_o.transpose(0, 3, 1, 2).reshape(mixed, -1)
        a_d_t = a_down.transpose(0, 2, 1).reshape(mixed, -1)

        gtile, dtile = 256, 512
        dma = pltpu.SemaphoreType.DMA
        exchange_scratch = Exchange.scratch(seq_len, width + LANES, width)
        own_rows = seq_len // 2 // CHIPS
        out, _ = pl.pallas_call(
            functools.partial(layer_kernel, count, scale, rank, n_q // head_dim, head_dim),
            out_shape=(jax.ShapeDtypeStruct(x_in.shape, BF16), jax.ShapeDtypeStruct(x_in.shape, BF16)),
            in_specs=[ANY] * 6 + [VMEM] * 10, out_specs=(ANY, ANY),
            scratch_shapes=exchange_scratch * 2 + [pltpu.VMEM((2, 4 * mixed, width), BF16)] + Gather.scratch() + [
                pltpu.VMEM((width, n_all), BF16), pltpu.VMEM((n_q, width), BF16),
                pltpu.VMEM((width // dtile, ff, dtile), BF16), pltpu.VMEM((3, width, gtile), BF16),
                pltpu.VMEM((seq_len, width), BF16), pltpu.VMEM((seq_len, n_all), BF16),
                pltpu.VMEM((seq_len, n_q), BF16), pltpu.VMEM((seq_len, ff), BF16),
                pltpu.VMEM((seq_len, 4 * mixed), BF16), pltpu.VMEM((count, own_rows, width), BF16),
                pltpu.VMEM((2, own_rows, width), BF16), dma((2,)), dma((width // dtile,)), dma((3,)), dma, dma,
                dma((2,))],
            compiler_params=pltpu.CompilerParams(collective_id=0, has_side_effects=True, vmem_limit_bytes=VMEM_LIMIT),
        )(x_in, w_all, w_o.reshape(-1, width), w_gate, w_up, w_down, own, b_qkv, b_g, b_u, a_o_t, a_d_t, masks[:, None], amask,
          gain_attn.reshape(1, -1), gain_mlp.reshape(1, -1))
        return out

    return jax.shard_map(local_layer, mesh=mesh, in_specs=in_specs, out_specs=act_spec, check_vma=False)
```

```python
import functools

import jax
import jax.numpy as jnp
from jax import lax
from jax.experimental import pallas as pl
from jax.experimental.pallas import tpu as pltpu
from jax.sharding import PartitionSpec as P

value_a10 = 16
RMS_EPS = 1e-5
F32 = jnp.float32
BF16 = jnp.bfloat16
MESH = pl.DeviceIdType.MESH
ANY = pl.BlockSpec(memory_space=pl.ANY)
VMEM = pl.BlockSpec(memory_space=pltpu.VMEM)
VMEM_LIMIT = 67043328
LANES = 128
CHIPS = 4
LAG = 3


class Exchange:
    def __init__(self, part, recv0, recv1, recv2, quart, done, out, sems):
        self.part, self.recv0, self.recv1, self.recv2 = part, recv0, recv1, recv2
        self.quart, self.done, self.out = quart, done, out
        (self.s0, self.r0, self.s1, self.r1, self.s2, self.r2, self.sa, self.ra, self.sb, self.rb, self.sc, self.rc,
         self.own) = sems
        me = lax.axis_index('tp')
        self.chip, self.core = me // 2, me % 2
        self.half = part.shape[0] // 2
        self.rows = self.half // CHIPS
        self.hrows = self.rows // 2
        self.right = self.device(self.chip + 1, self.core)
        self.left = self.device(self.chip + CHIPS - 1, self.core)
        self.partner = self.device(self.chip, 1 - self.core)

    def device(self, chip, core):
        return (chip % CHIPS) * 2 + core

    @staticmethod
    def scratch(seq_len, width, done_width):
        half = seq_len // 2
        rows = half // CHIPS
        dma = pltpu.SemaphoreType.DMA
        return [pltpu.VMEM((seq_len, width), BF16), pltpu.VMEM((2, half, width), BF16),
                pltpu.VMEM((2, 2, rows // 2, width), BF16), pltpu.VMEM((2, 2, rows, width), BF16),
                pltpu.VMEM((2, half, width), BF16), pltpu.VMEM((2, rows, done_width), BF16),
                dma((2,)), dma((2,)), dma((2, 2)), dma((2, 2)), dma((2, 2)), dma((2, 2)),
                dma((3, 2)), dma((3, 2)), dma((4, 2)), dma((4, 2)), dma((2,)), dma((2,)), dma((2,))]

    def barrier(self):
        sem = pltpu.get_barrier_semaphore()
        for other in (self.right, self.left, self.partner):
            pl.semaphore_signal(sem, inc=1, device_id={'tp': other}, device_id_type=MESH)
        pl.semaphore_wait(sem, 3)

    def send(self, src, dst, send_sem, recv_sem, other):
        return pltpu.make_async_remote_copy(src_ref=src, dst_ref=dst, send_sem=send_sem, recv_sem=recv_sem,
                                            device_id={'tp': other}, device_id_type=MESH)

    def slab(self, step):
        return pl.multiple_of(((self.chip + step) % CHIPS) * self.rows, self.rows)

    def own_row(self):
        return pl.multiple_of(self.core * self.half + self.slab(0), self.rows)

    def copy0(self, c):
        first = pl.multiple_of((1 - self.core) * self.half, self.half)
        return [self.send(self.part.at[pl.ds(first, self.half)], self.recv0.at[c % 2], self.s0.at[c % 2],
                          self.r0.at[c % 2], self.partner)]

    def copy1(self, c):
        quart, far = self.quart.at[c % 2], self.slab(2)
        low = pl.multiple_of(far + self.hrows, self.hrows)
        return [self.send(quart.at[pl.ds(far, self.hrows)], self.recv1.at[0, c % 2], self.s1.at[0, c % 2],
                          self.r1.at[0, c % 2], self.right),
                self.send(quart.at[pl.ds(low, self.hrows)], self.recv1.at[1, c % 2], self.s1.at[1, c % 2],
                          self.r1.at[1, c % 2], self.left)]

    def copy2(self, c):
        quart = self.quart.at[c % 2]
        return [self.send(quart.at[pl.ds(self.slab(1), self.rows)], self.recv2.at[0, c % 2], self.s2.at[0, c % 2],
                          self.r2.at[0, c % 2], self.right),
                self.send(quart.at[pl.ds(self.slab(CHIPS - 1), self.rows)], self.recv2.at[1, c % 2],
                          self.s2.at[1, c % 2], self.r2.at[1, c % 2], self.left)]

    def copy_a(self, c):
        dst = self.out.at[c, pl.ds(self.own_row(), self.rows)]
        return [self.send(self.done.at[c % 2], dst, self.sa.at[i, c % 2], self.ra.at[i, c % 2], other)
                for i, other in enumerate((self.right, self.left, self.partner))]

    def copy_own(self, c):
        return pltpu.make_async_copy(self.done.at[c % 2], self.out.at[c, pl.ds(self.own_row(), self.rows)],
                                     self.own.at[c % 2])

    def copy_b(self, c):
        base = self.core * self.half
        from_left = pl.multiple_of(base + self.slab(CHIPS - 1), self.rows)
        from_right = pl.multiple_of(base + self.slab(1), self.rows)
        low = pl.multiple_of(from_right + self.hrows, self.hrows)
        parts = ((from_left, self.hrows, self.right), (low, self.hrows, self.left),
                 (from_left, self.rows, self.partner), (from_right, self.rows, self.partner))
        return [self.send(self.out.at[c, pl.ds(first, size)], self.out.at[c, pl.ds(first, size)],
                          self.sb.at[i, c % 2], self.rb.at[i, c % 2], other)
                for i, (first, size, other) in enumerate(parts)]

    def copy_c(self, c):
        far = pl.multiple_of(self.core * self.half + self.slab(2), self.rows)
        rows = self.out.at[c, pl.ds(far, self.rows)]
        return [self.send(rows, rows, self.sc.at[c % 2], self.rc.at[c % 2], self.partner)]

    @staticmethod
    def start(copies):
        for copy in copies:
            copy.start()

    @staticmethod
    def wait_send(copies):
        for copy in copies:
            copy.wait_send()

    @staticmethod
    def wait_recv(copies):
        for copy in copies:
            copy.wait_recv()

    def add_pair(self, c):
        self.wait_recv(self.copy0(c))
        self.wait_send(self.copy0(c))
        quart, recv = self.quart.at[c % 2], self.recv0.at[c % 2]
        own = self.core * self.half

        @pl.loop(0, self.half // 16)
        def _(i):
            mine = self.part[pl.ds(pl.multiple_of(own + i * 16, 16), 16), :].astype(F32)
            rows = pl.ds(pl.multiple_of(i * 16, 16), 16)
            quart[rows, :] = (mine + recv[rows, :].astype(F32)).astype(BF16)

        self.start(self.copy1(c))

    def add_far(self, c):
        self.wait_recv(self.copy1(c))
        quart = self.quart.at[c % 2]
        for side, first in ((0, self.slab(1)), (1, self.slab(CHIPS - 1) + self.hrows)):
            rows = pl.ds(pl.multiple_of(first, self.hrows), self.hrows)
            quart[rows, :] = (quart[rows, :].astype(F32) + self.recv1[side, c % 2].astype(F32)).astype(BF16)
        self.start(self.copy2(c))

    def finish(self, c, finalize):
        self.wait_recv(self.copy2(c))
        self.wait_send(self.copy1(c))
        quart, slot = self.quart.at[c % 2], c % 2

        def total(first, size, columns):
            rows = pl.ds(pl.multiple_of(self.slab(0) + first, size), size)
            here = pl.ds(first, size)
            return (quart[rows, columns].astype(F32) + self.recv2[0, slot, here, columns].astype(F32)
                    + self.recv2[1, slot, here, columns].astype(F32))

        finalize(c, total, self.done.at[slot])
        self.start(self.copy_a(c))
        self.copy_own(c).start()

    def forward(self, c):
        self.wait_recv(self.copy_a(c))
        self.wait_send(self.copy2(c))
        self.start(self.copy_b(c))

    def cross(self, c):
        self.wait_recv(self.copy_b(c))
        self.wait_send(self.copy_a(c))
        self.copy_own(c).wait()
        self.start(self.copy_c(c))

    def close(self, c):
        self.wait_recv(self.copy_c(c))
        self.wait_send(self.copy_b(c))
        self.wait_send(self.copy_c(c))

    def first_stages(self, slot, count, finalize):
        self.run(slot, count, ((2, self.cross), (1, lambda c: self.finish(c, finalize)), (0, self.add_pair)))

    def second_stages(self, slot, count, prefetch):
        def far(c):
            prefetch(c)
            self.add_far(c)

        self.run(slot, count, ((3, self.close), (2, self.forward), (1, far)))

    @staticmethod
    def run(slot, count, table):
        for lag, stage in table:
            @pl.when((slot >= lag) & (slot < count + lag))
            def _(lag=lag, stage=stage):
                stage(slot - lag)


class Gather:
    def __init__(self, exchange, own, full, sems):
        self.ex, self.own, self.full = exchange, own, full
        self.sa, self.ra, self.sb, self.rb, self.sc, self.rc = sems
        self.rows = own.shape[1]
        self.half = self.rows // 2

    @staticmethod
    def scratch():
        dma = pltpu.SemaphoreType.DMA
        return [dma((2, 3)), dma((2, 3)), dma((2, 4)), dma((2, 4)), dma((2,)), dma((2,))]

    def first(self, device):
        return pl.multiple_of(device * self.rows, self.rows)

    def copy_a(self, p):
        ex = self.ex
        dst = self.full.at[p, pl.ds(self.first(ex.device(ex.chip, ex.core)), self.rows)]
        return [ex.send(self.own.at[p], dst, self.sa.at[p, i], self.ra.at[p, i], other)
                for i, other in enumerate((ex.right, ex.left, ex.partner))]

    def copy_b(self, p):
        ex = self.ex
        from_left, from_right = self.first(ex.left), self.first(ex.right)
        low = pl.multiple_of(from_right + self.half, self.half)
        parts = ((from_left, self.half, ex.right), (low, self.half, ex.left),
                 (from_left, self.rows, ex.partner), (from_right, self.rows, ex.partner))
        return [ex.send(self.full.at[p, pl.ds(first, size)], self.full.at[p, pl.ds(first, size)], self.sb.at[p, i],
                        self.rb.at[p, i], other) for i, (first, size, other) in enumerate(parts)]

    def copy_c(self, p):
        ex = self.ex
        rows = self.full.at[p, pl.ds(self.first(ex.device(ex.chip + 2, ex.core)), self.rows)]
        return [ex.send(rows, rows, self.sc.at[p], self.rc.at[p], ex.partner)]

    def begin(self, p):
        me = self.ex.device(self.ex.chip, self.ex.core)
        self.ex.start(self.copy_a(p))
        self.full[p, pl.ds(self.first(me), self.rows), :] = self.own[p]

    def forward(self, p):
        self.ex.wait_recv(self.copy_a(p))
        self.ex.start(self.copy_b(p))

    def cross(self, p):
        self.ex.wait_recv(self.copy_b(p))
        self.ex.start(self.copy_c(p))

    def close(self, p):
        self.ex.wait_recv(self.copy_c(p))
        for copies in (self.copy_a, self.copy_b, self.copy_c):
            self.ex.wait_send(copies(p))


def dot_t(a, b):
    return lax.dot_general(a, b, (((1,), (1,)), ((), ())), preferred_element_type=F32)


def dot(a, b):
    return jnp.dot(a, b, preferred_element_type=F32)


def layer_kernel(count, scale, rank, heads, head_dim, x_ref, wqkv_ref, wo_ref, wg_ref, wu_ref, wd_ref, own_ref,
                 bqkv_ref, bg_ref, bu_ref, ao_ref, ad_ref, masks_ref, amask_ref, gain_a_ref, gain_m_ref, y_ref, h2_ref,
                 *scratch):
    one = Exchange(*scratch[:6], h2_ref, scratch[6:19])
    two = Exchange(*scratch[19:25], y_ref, scratch[25:38])
    full = scratch[38]
    gather = Gather(one, own_ref, full, scratch[39:45])
    (wqkv, wo, wd, ring, ubuf, qkv, att, mid, t_buf, x1, rbuf, sem_w, sem_d, sem_ring, sem_x, sem_h, sem_r) = scratch[45:]
    seq_len, width = ubuf.shape
    gtile, dtile = ring.shape[2], wd.shape[2]
    pairs, downs = mid.shape[1] // gtile, wd.shape[0]
    otile = 1024
    mixed = full.shape[1]

    def load_x(c):
        return pltpu.make_async_copy(x_ref.at[c], ubuf, sem_x)

    def load_h(c):
        return pltpu.make_async_copy(h2_ref.at[c], ubuf, sem_h)

    def load_r(c):
        return pltpu.make_async_copy(x_ref.at[c, pl.ds(one.own_row(), one.rows)], rbuf.at[c % 2], sem_r.at[c % 2])

    def load_d(n):
        columns = pl.ds(pl.multiple_of(n * dtile, dtile), dtile)
        return pltpu.make_async_copy(wd_ref.at[:, columns], wd.at[n], sem_d.at[n])

    def load_tile(w_ref, c, j, side):
        place = ((c * pairs + j) * 2 + side) % 3
        columns = pl.ds(pl.multiple_of(j * gtile, gtile), gtile)
        return pltpu.make_async_copy(w_ref.at[:, columns], ring.at[place], sem_ring.at[place]), place

    load_qkv = pltpu.make_async_copy(wqkv_ref, wqkv, sem_w.at[0])
    load_o = pltpu.make_async_copy(wo_ref, wo, sem_w.at[1])

    load_x(0).start()
    load_qkv.start()
    load_o.start()
    one.barrier()
    gather.begin(0)
    gather.begin(1)
    for w_ref, j, side in ((wg_ref, 0, 0), (wu_ref, 0, 1), (wg_ref, 1, 0)):
        load_tile(w_ref, 0, j, side)[0].start()
    for n in range(downs):
        load_d(n).start()

    def attention(c):
        load_x(c).wait()

        @pl.loop(0, seq_len // 64)
        def _(i):
            rows = pl.ds(pl.multiple_of(i * 64, 64), 64)
            square = jnp.zeros((64, LANES), F32)
            for n in range(width // LANES):
                value = ubuf[rows, n * LANES:(n + 1) * LANES].astype(F32)
                square += value * value
            inv_rms = lax.rsqrt(jnp.sum(square, axis=1, keepdims=True) / width + RMS_EPS)
            for n in range(width // LANES):
                columns = pl.ds(n * LANES, LANES)
                ubuf[rows, columns] = (ubuf[rows, columns].astype(F32) * inv_rms * gain_a_ref[:, columns]).astype(BF16)

        @pl.when(c == 0)
        def _():
            gather.forward(0)
            gather.cross(0)
            load_qkv.wait()
            load_o.wait()
            gather.close(0)

        @pl.when(c == 1)
        def _():
            gather.close(1)

        keep = masks_ref[c, :, 0:mixed] > 0
        t_buf[...] = jnp.where(keep, dot_t(ubuf[...], full[0]).astype(BF16).astype(F32), 0.0).astype(BF16)

        @pl.loop(0, qkv.shape[1] // 256)
        def _(n):
            columns = pl.ds(pl.multiple_of(n * 256, 256), 256)
            base = dot(ubuf[...], wqkv[:, columns])
            qkv[:, columns] = (base + scale * dot(t_buf[...], bqkv_ref[:, columns])).astype(BF16)

        @pl.when(c >= LAG)
        def _():
            load_h(c - LAG).start()

        @pl.when((c + 1 < count) & (c < LAG))
        def _():
            load_x(c + 1).start()

        @pl.when(c == 0)
        def _():
            gather.forward(1)

        kv_heads = (qkv.shape[1] // head_dim - heads) // 2
        causal = (lax.broadcasted_iota(jnp.int32, (seq_len, seq_len), 0)
                  >= lax.broadcasted_iota(jnp.int32, (seq_len, seq_len), 1))
        for j in range(heads):
            kv = heads + j * kv_heads // heads
            query, key, value = (qkv[:, i * head_dim:(i + 1) * head_dim] for i in (j, kv, kv + kv_heads))
            scores = jnp.where(causal, dot_t(query, key) * head_dim ** -0.5, -jnp.inf)
            prob = jnp.exp(scores - jnp.max(scores, axis=1, keepdims=True))
            prob = (prob / jnp.sum(prob, axis=1, keepdims=True)).astype(BF16)
            att[:, j * head_dim:(j + 1) * head_dim] = dot(prob, value).astype(BF16)

        @pl.loop(0, width // otile)
        def _(n):
            columns = pl.ds(pl.multiple_of(n * otile, otile), otile)
            one.part[:, columns] = dot(att[...], wo[:, columns]).astype(BF16)

        pad = jnp.zeros((seq_len, LANES - ao_ref.shape[0]), F32)
        one.part[:, width:] = jnp.concatenate([dot_t(att[...], ao_ref[...]), pad], 1).astype(BF16)

        @pl.when(c == 0)
        def _():
            gather.cross(1)

    def mlp_start(c):
        load_h(c).wait()
        keep = masks_ref[c, :, mixed:2 * mixed] > 0
        t_buf[...] = jnp.where(keep, dot_t(ubuf[...], full[1]).astype(BF16).astype(F32), 0.0).astype(BF16)

    def gate_up(c, begin, end):
        def product(w_ref, b_ref, j, side):
            copy, place = load_tile(w_ref, c, j, side)
            copy.wait()
            columns = pl.ds(pl.multiple_of(j * gtile, gtile), gtile)
            out = dot(ubuf[...], ring[place]) + scale * dot(t_buf[...], b_ref[:, columns])
            return out.astype(BF16)

        def refill(w_ref, j, side):
            wrap = j // pairs
            @pl.when(c + wrap < count)
            def _():
                load_tile(w_ref, c + wrap, j % pairs, side)[0].start()

        @pl.loop(begin, end)
        def _(j):
            columns = pl.ds(pl.multiple_of(j * gtile, gtile), gtile)
            mid[:, columns] = product(wg_ref, bg_ref, j, 0)
            refill(wu_ref, j + 1, 1)
            up = product(wu_ref, bu_ref, j, 1)
            refill(wg_ref, j + 2, 0)
            mid[:, columns] = (jax.nn.silu(mid[:, columns].astype(F32)) * up.astype(F32)).astype(BF16)

    def down(c):
        @pl.when(c + LAG + 1 < count)
        def _():
            load_x(c + LAG + 1).start()

        @pl.loop(0, downs)
        def _(n):
            @pl.when(c == 0)
            def _():
                load_d(n).wait()
            columns = pl.ds(pl.multiple_of(n * dtile, dtile), dtile)
            two.part[:, columns] = dot(mid[...], wd[n]).astype(BF16)

        pad = jnp.zeros((seq_len, LANES - ad_ref.shape[0]), F32)
        two.part[:, width:] = jnp.concatenate([dot_t(mid[...], ad_ref[...]), pad], 1).astype(BF16)

    def totals(c, total, exchange, first_b):
        tile = width // (mixed // own_ref.shape[1])
        lanes = total(0, exchange.rows, pl.ds(width, LANES)).astype(BF16).astype(F32)
        lane = lax.broadcasted_iota(jnp.int32, lanes.shape, 1)
        keep = masks_ref[c, :, 2 * mixed:2 * mixed + LANES] > 0
        lanes = jnp.where(keep, lanes, 0.0)
        columns = [jnp.sum(jnp.where(lane % rank == r, lanes, 0.0), axis=1, keepdims=True) for r in range(rank)]
        chosen = amask_ref[c] > 0
        for n in range(width // tile):
            lora = None
            for r in range(rank):
                b_all = full[1, n * own_ref.shape[1] + first_b:n * own_ref.shape[1] + first_b + 8,
                             r * tile:(r + 1) * tile].astype(F32)
                b_row = jnp.sum(jnp.where(chosen[:, :1], b_all, 0.0), axis=0, keepdims=True)
                lora = columns[r] * b_row if lora is None else lora + columns[r] * b_row
            yield pl.ds(n * tile, tile), total(0, exchange.rows, pl.ds(n * tile, tile)) + scale * lora

    def finish_one(c, total, done):
        load_r(c).wait()
        square = jnp.zeros((one.rows, 1), F32)
        for columns, z_out in totals(c, total, one, 16):
            x_one = (rbuf[c % 2, :, columns].astype(F32) + z_out).astype(BF16)
            x1[c, :, columns] = x_one
            x_one = x_one.astype(F32)
            square += jnp.sum(x_one * x_one, axis=1, keepdims=True)
        inv_rms = lax.rsqrt(square / width + RMS_EPS)
        for n in range(width // 512):
            columns = pl.ds(n * 512, 512)
            done[:, columns] = (x1[c, :, columns].astype(F32) * inv_rms * gain_m_ref[:, columns]).astype(BF16)

    def finish_two(c, total, done):
        for columns, z_out in totals(c, total, two, 24):
            done[:, columns] = (x1[c, :, columns].astype(F32) + z_out).astype(BF16)

    split = pairs // 2

    @pl.loop(0, count + 2 * LAG)
    def _(slot):
        late = slot - LAG
        busy = (slot >= LAG) & (slot < count + LAG)
        one.second_stages(slot, count, lambda c: load_r(c).start())

        @pl.when((slot >= count) & busy)
        def _():
            load_h(late).start()

        two.first_stages(late - 1, count, finish_two)

        @pl.when(slot < count)
        def _():
            attention(slot)
            one.start(one.copy0(slot))

        @pl.when(busy)
        def _():
            mlp_start(late)
            gate_up(late, 0, split)

        one.first_stages(slot, count, finish_one)
        two.second_stages(late, count, lambda c: None)

        @pl.when(busy)
        def _():
            gate_up(late, split, pairs)
            down(late)
            two.start(two.copy0(late))


def solution(mesh):
    act_spec = P('dp', None, None)
    w_head_spec = P(None, 'tp', None)
    w_out_spec = P('tp', None, None)
    w_col_spec = P(None, 'tp')
    w_row_spec = P('tp', None)
    a_rank_spec = P(None, None, 'tp')
    b_head_spec = P(None, None, 'tp', None)
    b_col_spec = P(None, None, 'tp')
    a_head_spec = P(None, 'tp', None, None)
    a_row_spec = P(None, 'tp', None)
    in_specs = (act_spec, P('dp'), P(None), P(None), w_head_spec, w_head_spec, w_head_spec, w_out_spec,
                w_col_spec, w_col_spec, w_row_spec, a_rank_spec, b_head_spec, a_rank_spec, b_head_spec,
                a_rank_spec, b_head_spec, a_head_spec, b_col_spec, a_rank_spec, b_col_spec,
                a_rank_spec, b_col_spec, a_row_spec, b_col_spec)

    def local_layer(x_in, adapter_ids, gain_attn, gain_mlp, w_q, w_k, w_v, w_o, w_gate, w_up, w_down,
                    a_q, b_q, a_k, b_k, a_v, b_v, a_o, b_o, a_gate, b_gate, a_up, b_up, a_down, b_down):
        count, seq_len, width = x_in.shape
        adapters, rank = b_q.shape[:2]
        mixed = adapters * rank
        scale = value_a10 / rank
        ff = w_gate.shape[1]

        group = mesh.shape['tp']
        head_dim = w_k.shape[2]
        n_q, n_k = w_q[0].size, w_k[0].size

        def plane(b):
            return b.transpose(1, 0, 2).reshape(group, adapters, -1)

        def planes(parts):
            zero = jnp.zeros_like(parts[0])
            return jnp.stack(list(parts) + [zero] * (4 - len(parts)), 1).reshape(4 * mixed, -1)

        a_loc = [a.transpose(2, 0, 1).reshape(adapters, width) for a in (a_q, a_k, a_v, a_gate, a_up)]
        b_loc = [b.reshape(adapters, -1) for b in (b_o, b_down)]
        own = jnp.stack([jnp.concatenate(a_loc[:3] + [jnp.zeros_like(a_loc[0])], 0),
                         jnp.concatenate(a_loc[3:] + b_loc, 0)])
        b_in = [plane(b.reshape(adapters, rank, -1)) for b in (b_q, b_k, b_v)]
        n_all = n_q + 2 * n_k
        b_qkv = planes([jnp.pad(b, ((0, 0), (0, 0), (at, n_all - at - b.shape[2])))
                        for b, at in zip(b_in, (0, n_q, n_q + n_k))])
        b_g = planes([plane(b_gate)])
        b_u = planes([jnp.zeros_like(plane(b_up)), plane(b_up)])

        index = jnp.arange(4 * mixed)
        mine = index % adapters == adapter_ids[:, None]
        index_plane = index // adapters % 4
        lane = jnp.arange(LANES)
        masks = jnp.concatenate([mine & (index_plane < 3), mine & (index_plane < 2),
                                 lane // rank == adapter_ids[:, None]], 1).astype(F32)
        amask = jnp.broadcast_to((jnp.arange(adapters) == adapter_ids[:, None])[:, :, None].astype(F32),
                                 (count, adapters, LANES))
        w_all = jnp.concatenate([w.reshape(width, -1) for w in (w_q, w_k, w_v)], 1)
        a_o_t = a_o.transpose(0, 3, 1, 2).reshape(mixed, -1)
        a_d_t = a_down.transpose(0, 2, 1).reshape(mixed, -1)

        gtile, dtile = 256, 1024
        dma = pltpu.SemaphoreType.DMA
        exchange_scratch = Exchange.scratch(seq_len, width + LANES, width)
        own_rows = seq_len // 2 // CHIPS
        out, _ = pl.pallas_call(
            functools.partial(layer_kernel, count, scale, rank, n_q // head_dim, head_dim),
            out_shape=(jax.ShapeDtypeStruct(x_in.shape, BF16), jax.ShapeDtypeStruct(x_in.shape, BF16)),
            in_specs=[ANY] * 6 + [VMEM] * 10, out_specs=(ANY, ANY),
            scratch_shapes=exchange_scratch * 2 + [pltpu.VMEM((2, 4 * mixed, width), BF16)] + Gather.scratch() + [
                pltpu.VMEM((width, n_all), BF16), pltpu.VMEM((n_q, width), BF16),
                pltpu.VMEM((width // dtile, ff, dtile), BF16), pltpu.VMEM((3, width, gtile), BF16),
                pltpu.VMEM((seq_len, width), BF16), pltpu.VMEM((seq_len, n_all), BF16),
                pltpu.VMEM((seq_len, n_q), BF16), pltpu.VMEM((seq_len, ff), BF16),
                pltpu.VMEM((seq_len, 4 * mixed), BF16), pltpu.VMEM((count, own_rows, width), BF16),
                pltpu.VMEM((2, own_rows, width), BF16), dma((2,)), dma((width // dtile,)), dma((3,)), dma, dma,
                dma((2,))],
            compiler_params=pltpu.CompilerParams(collective_id=0, has_side_effects=True, vmem_limit_bytes=VMEM_LIMIT),
        )(x_in, w_all, w_o.reshape(-1, width), w_gate, w_up, w_down, own, b_qkv, b_g, b_u, a_o_t, a_d_t, masks[:, None], amask,
          gain_attn.reshape(1, -1), gain_mlp.reshape(1, -1))
        return out

    return jax.shard_map(local_layer, mesh=mesh, in_specs=in_specs, out_specs=act_spec, check_vma=False)
```

```python
import functools

import jax
import jax.numpy as jnp
from jax import lax
from jax.experimental import pallas as pl
from jax.experimental.pallas import tpu as pltpu
from jax.sharding import PartitionSpec as P

value_a10 = 16
RMS_EPS = 1e-5
F32 = jnp.float32
BF16 = jnp.bfloat16
MESH = pl.DeviceIdType.MESH
ANY = pl.BlockSpec(memory_space=pl.ANY)
VMEM = pl.BlockSpec(memory_space=pltpu.VMEM)
VMEM_LIMIT = 67043328
LANES = 128
CHIPS = 4
LAG = 3


class Exchange:
    def __init__(self, part, recv0, recv1, recv2, quart, done, out, sems):
        self.part, self.recv0, self.recv1, self.recv2 = part, recv0, recv1, recv2
        self.quart, self.done, self.out = quart, done, out
        (self.s0, self.r0, self.s1, self.r1, self.s2, self.r2, self.sa, self.ra, self.sb, self.rb, self.sc, self.rc,
         self.own) = sems
        me = lax.axis_index('tp')
        self.chip, self.core = me // 2, me % 2
        self.half = part.shape[0] // 2
        self.rows = self.half // CHIPS
        self.hrows = self.rows // 2
        self.right = self.device(self.chip + 1, self.core)
        self.left = self.device(self.chip + CHIPS - 1, self.core)
        self.partner = self.device(self.chip, 1 - self.core)

    def device(self, chip, core):
        return (chip % CHIPS) * 2 + core

    @staticmethod
    def scratch(seq_len, width, done_width):
        half = seq_len // 2
        rows = half // CHIPS
        dma = pltpu.SemaphoreType.DMA
        return [pltpu.VMEM((seq_len, width), BF16), pltpu.VMEM((2, half, width), BF16),
                pltpu.VMEM((2, 2, rows // 2, width), BF16), pltpu.VMEM((2, 2, rows, width), BF16),
                pltpu.VMEM((2, half, width), BF16), pltpu.VMEM((2, rows, done_width), BF16),
                dma((2,)), dma((2,)), dma((2, 2)), dma((2, 2)), dma((2, 2)), dma((2, 2)),
                dma((3, 2)), dma((3, 2)), dma((4, 2)), dma((4, 2)), dma((2,)), dma((2,)), dma((2,))]

    def barrier(self):
        sem = pltpu.get_barrier_semaphore()
        for other in (self.right, self.left, self.partner):
            pl.semaphore_signal(sem, inc=1, device_id={'tp': other}, device_id_type=MESH)
        pl.semaphore_wait(sem, 3)

    def send(self, src, dst, send_sem, recv_sem, other):
        return pltpu.make_async_remote_copy(src_ref=src, dst_ref=dst, send_sem=send_sem, recv_sem=recv_sem,
                                            device_id={'tp': other}, device_id_type=MESH)

    def slab(self, step):
        return pl.multiple_of(((self.chip + step) % CHIPS) * self.rows, self.rows)

    def own_row(self):
        return pl.multiple_of(self.core * self.half + self.slab(0), self.rows)

    def copy0(self, c):
        first = pl.multiple_of((1 - self.core) * self.half, self.half)
        return [self.send(self.part.at[pl.ds(first, self.half)], self.recv0.at[c % 2], self.s0.at[c % 2],
                          self.r0.at[c % 2], self.partner)]

    def copy1(self, c):
        quart, far = self.quart.at[c % 2], self.slab(2)
        low = pl.multiple_of(far + self.hrows, self.hrows)
        return [self.send(quart.at[pl.ds(far, self.hrows)], self.recv1.at[0, c % 2], self.s1.at[0, c % 2],
                          self.r1.at[0, c % 2], self.right),
                self.send(quart.at[pl.ds(low, self.hrows)], self.recv1.at[1, c % 2], self.s1.at[1, c % 2],
                          self.r1.at[1, c % 2], self.left)]

    def copy2(self, c):
        quart = self.quart.at[c % 2]
        return [self.send(quart.at[pl.ds(self.slab(1), self.rows)], self.recv2.at[0, c % 2], self.s2.at[0, c % 2],
                          self.r2.at[0, c % 2], self.right),
                self.send(quart.at[pl.ds(self.slab(CHIPS - 1), self.rows)], self.recv2.at[1, c % 2],
                          self.s2.at[1, c % 2], self.r2.at[1, c % 2], self.left)]

    def copy_a(self, c):
        dst = self.out.at[c, pl.ds(self.own_row(), self.rows)]
        return [self.send(self.done.at[c % 2], dst, self.sa.at[i, c % 2], self.ra.at[i, c % 2], other)
                for i, other in enumerate((self.right, self.left, self.partner))]

    def copy_own(self, c):
        return pltpu.make_async_copy(self.done.at[c % 2], self.out.at[c, pl.ds(self.own_row(), self.rows)],
                                     self.own.at[c % 2])

    def copy_b(self, c):
        base = self.core * self.half
        from_left = pl.multiple_of(base + self.slab(CHIPS - 1), self.rows)
        from_right = pl.multiple_of(base + self.slab(1), self.rows)
        low = pl.multiple_of(from_right + self.hrows, self.hrows)
        parts = ((from_left, self.hrows, self.right), (low, self.hrows, self.left),
                 (from_left, self.rows, self.partner), (from_right, self.rows, self.partner))
        return [self.send(self.out.at[c, pl.ds(first, size)], self.out.at[c, pl.ds(first, size)],
                          self.sb.at[i, c % 2], self.rb.at[i, c % 2], other)
                for i, (first, size, other) in enumerate(parts)]

    def copy_c(self, c):
        far = pl.multiple_of(self.core * self.half + self.slab(2), self.rows)
        rows = self.out.at[c, pl.ds(far, self.rows)]
        return [self.send(rows, rows, self.sc.at[c % 2], self.rc.at[c % 2], self.partner)]

    @staticmethod
    def start(copies):
        for copy in copies:
            copy.start()

    @staticmethod
    def wait_send(copies):
        for copy in copies:
            copy.wait_send()

    @staticmethod
    def wait_recv(copies):
        for copy in copies:
            copy.wait_recv()

    def add_pair(self, c):
        self.wait_recv(self.copy0(c))
        self.wait_send(self.copy0(c))
        quart, recv = self.quart.at[c % 2], self.recv0.at[c % 2]
        own = self.core * self.half

        @pl.loop(0, self.half // 16)
        def _(i):
            mine = self.part[pl.ds(pl.multiple_of(own + i * 16, 16), 16), :].astype(F32)
            rows = pl.ds(pl.multiple_of(i * 16, 16), 16)
            quart[rows, :] = (mine + recv[rows, :].astype(F32)).astype(BF16)

        self.start(self.copy1(c))

    def add_far(self, c):
        self.wait_recv(self.copy1(c))
        quart = self.quart.at[c % 2]
        for side, first in ((0, self.slab(1)), (1, self.slab(CHIPS - 1) + self.hrows)):
            rows = pl.ds(pl.multiple_of(first, self.hrows), self.hrows)
            quart[rows, :] = (quart[rows, :].astype(F32) + self.recv1[side, c % 2].astype(F32)).astype(BF16)
        self.start(self.copy2(c))

    def finish(self, c, finalize):
        self.wait_recv(self.copy2(c))
        self.wait_send(self.copy1(c))
        quart, slot = self.quart.at[c % 2], c % 2

        def total(first, size, columns):
            rows = pl.ds(pl.multiple_of(self.slab(0) + first, size), size)
            here = pl.ds(first, size)
            return (quart[rows, columns].astype(F32) + self.recv2[0, slot, here, columns].astype(F32)
                    + self.recv2[1, slot, here, columns].astype(F32))

        finalize(c, total, self.done.at[slot])
        self.start(self.copy_a(c))
        self.copy_own(c).start()

    def forward(self, c):
        self.wait_recv(self.copy_a(c))
        self.wait_send(self.copy2(c))
        self.start(self.copy_b(c))

    def cross(self, c):
        self.wait_recv(self.copy_b(c))
        self.wait_send(self.copy_a(c))
        self.copy_own(c).wait()
        self.start(self.copy_c(c))

    def close(self, c):
        self.wait_recv(self.copy_c(c))
        self.wait_send(self.copy_b(c))
        self.wait_send(self.copy_c(c))

    def first_stages(self, slot, count, finalize):
        self.run(slot, count, ((2, self.cross), (1, lambda c: self.finish(c, finalize)), (0, self.add_pair)))

    def second_stages(self, slot, count, prefetch):
        def far(c):
            prefetch(c)
            self.add_far(c)

        self.run(slot, count, ((3, self.close), (2, self.forward), (1, far)))

    @staticmethod
    def run(slot, count, table):
        for lag, stage in table:
            @pl.when((slot >= lag) & (slot < count + lag))
            def _(lag=lag, stage=stage):
                stage(slot - lag)


class Gather:
    def __init__(self, exchange, own, full, sems):
        self.ex, self.own, self.full = exchange, own, full
        self.sa, self.ra, self.sb, self.rb, self.sc, self.rc = sems
        self.rows = own.shape[1]
        self.half = self.rows // 2

    @staticmethod
    def scratch():
        dma = pltpu.SemaphoreType.DMA
        return [dma((2, 3)), dma((2, 3)), dma((2, 4)), dma((2, 4)), dma((2,)), dma((2,))]

    def first(self, device):
        return pl.multiple_of(device * self.rows, self.rows)

    def copy_a(self, p):
        ex = self.ex
        dst = self.full.at[p, pl.ds(self.first(ex.device(ex.chip, ex.core)), self.rows)]
        return [ex.send(self.own.at[p], dst, self.sa.at[p, i], self.ra.at[p, i], other)
                for i, other in enumerate((ex.right, ex.left, ex.partner))]

    def copy_b(self, p):
        ex = self.ex
        from_left, from_right = self.first(ex.left), self.first(ex.right)
        low = pl.multiple_of(from_right + self.half, self.half)
        parts = ((from_left, self.half, ex.right), (low, self.half, ex.left),
                 (from_left, self.rows, ex.partner), (from_right, self.rows, ex.partner))
        return [ex.send(self.full.at[p, pl.ds(first, size)], self.full.at[p, pl.ds(first, size)], self.sb.at[p, i],
                        self.rb.at[p, i], other) for i, (first, size, other) in enumerate(parts)]

    def copy_c(self, p):
        ex = self.ex
        rows = self.full.at[p, pl.ds(self.first(ex.device(ex.chip + 2, ex.core)), self.rows)]
        return [ex.send(rows, rows, self.sc.at[p], self.rc.at[p], ex.partner)]

    def begin(self, p):
        me = self.ex.device(self.ex.chip, self.ex.core)
        self.ex.start(self.copy_a(p))
        self.full[p, pl.ds(self.first(me), self.rows), :] = self.own[p]

    def forward(self, p):
        self.ex.wait_recv(self.copy_a(p))
        self.ex.start(self.copy_b(p))

    def cross(self, p):
        self.ex.wait_recv(self.copy_b(p))
        self.ex.start(self.copy_c(p))

    def close(self, p):
        self.ex.wait_recv(self.copy_c(p))
        for copies in (self.copy_a, self.copy_b, self.copy_c):
            self.ex.wait_send(copies(p))


def dot_t(a, b):
    return lax.dot_general(a, b, (((1,), (1,)), ((), ())), preferred_element_type=F32)


def dot(a, b):
    return jnp.dot(a, b, preferred_element_type=F32)


def layer_kernel(count, scale, rank, heads, head_dim, x_ref, wqkv_ref, wo_ref, wg_ref, wu_ref, wd_ref, own_ref,
                 bqkv_ref, bg_ref, bu_ref, ao_ref, ad_ref, masks_ref, amask_ref, gain_a_ref, gain_m_ref, y_ref, h2_ref,
                 *scratch):
    one = Exchange(*scratch[:6], h2_ref, scratch[6:19])
    two = Exchange(*scratch[19:25], y_ref, scratch[25:38])
    full = scratch[38]
    gather = Gather(one, own_ref, full, scratch[39:45])
    (wqkv, wo, wd, ring, ubuf, qkv, att, mid, t_buf, x1, rbuf, sem_w, sem_d, sem_ring, sem_x, sem_h, sem_r) = scratch[45:]
    seq_len, width = ubuf.shape
    gtile, dtile = ring.shape[2], wd.shape[2]
    pairs, downs = mid.shape[1] // gtile, wd.shape[0]
    otile = 1024
    mixed = full.shape[1]

    def load_x(c):
        return pltpu.make_async_copy(x_ref.at[c], ubuf, sem_x)

    def load_h(c):
        return pltpu.make_async_copy(h2_ref.at[c], ubuf, sem_h)

    def load_r(c):
        return pltpu.make_async_copy(x_ref.at[c, pl.ds(one.own_row(), one.rows)], rbuf.at[c % 2], sem_r.at[c % 2])

    def load_d(n):
        columns = pl.ds(pl.multiple_of(n * dtile, dtile), dtile)
        return pltpu.make_async_copy(wd_ref.at[:, columns], wd.at[n], sem_d.at[n])

    def load_tile(w_ref, c, j, side):
        place = ((c * pairs + j) * 2 + side) % 3
        columns = pl.ds(pl.multiple_of(j * gtile, gtile), gtile)
        return pltpu.make_async_copy(w_ref.at[:, columns], ring.at[place], sem_ring.at[place]), place

    load_qkv = pltpu.make_async_copy(wqkv_ref, wqkv, sem_w.at[0])
    load_o = pltpu.make_async_copy(wo_ref, wo, sem_w.at[1])

    load_x(0).start()
    load_qkv.start()
    load_o.start()
    one.barrier()
    gather.begin(0)
    gather.begin(1)

    def attention(c):
        load_x(c).wait()

        @pl.loop(0, seq_len // 64)
        def _(i):
            rows = pl.ds(pl.multiple_of(i * 64, 64), 64)
            square = jnp.zeros((64, LANES), F32)
            for n in range(width // LANES):
                value = ubuf[rows, n * LANES:(n + 1) * LANES].astype(F32)
                square += value * value
            inv_rms = lax.rsqrt(jnp.sum(square, axis=1, keepdims=True) / width + RMS_EPS)
            for n in range(width // LANES):
                columns = pl.ds(n * LANES, LANES)
                ubuf[rows, columns] = (ubuf[rows, columns].astype(F32) * inv_rms * gain_a_ref[:, columns]).astype(BF16)

        @pl.when(c == 0)
        def _():
            gather.forward(0)
            gather.cross(0)
            load_qkv.wait()
            gather.close(0)

        @pl.when(c == 1)
        def _():
            gather.close(1)

        keep = masks_ref[c, :, 0:mixed] > 0
        t_buf[...] = jnp.where(keep, dot_t(ubuf[...], full[0]).astype(BF16).astype(F32), 0.0).astype(BF16)

        @pl.loop(0, qkv.shape[1] // 256)
        def _(n):
            columns = pl.ds(pl.multiple_of(n * 256, 256), 256)
            base = dot(ubuf[...], wqkv[:, columns])
            qkv[:, columns] = (base + scale * dot(t_buf[...], bqkv_ref[:, columns])).astype(BF16)

        @pl.when(c >= LAG)
        def _():
            load_h(c - LAG).start()

        @pl.when((c + 1 < count) & (c < LAG))
        def _():
            load_x(c + 1).start()

        @pl.when(c == 0)
        def _():
            gather.forward(1)
            load_o.wait()
            for w_ref, j, side in ((wg_ref, 0, 0), (wu_ref, 0, 1), (wg_ref, 1, 0)):
                load_tile(w_ref, 0, j, side)[0].start()
            for n in range(downs):
                load_d(n).start()

        kv_heads = (qkv.shape[1] // head_dim - heads) // 2
        causal = (lax.broadcasted_iota(jnp.int32, (seq_len, seq_len), 0)
                  >= lax.broadcasted_iota(jnp.int32, (seq_len, seq_len), 1))
        for j in range(heads):
            kv = heads + j * kv_heads // heads
            query, key, value = (qkv[:, i * head_dim:(i + 1) * head_dim] for i in (j, kv, kv + kv_heads))
            scores = jnp.where(causal, dot_t(query, key) * head_dim ** -0.5, -jnp.inf)
            prob = jnp.exp(scores - jnp.max(scores, axis=1, keepdims=True))
            prob = (prob / jnp.sum(prob, axis=1, keepdims=True)).astype(BF16)
            att[:, j * head_dim:(j + 1) * head_dim] = dot(prob, value).astype(BF16)

        @pl.loop(0, width // otile)
        def _(n):
            columns = pl.ds(pl.multiple_of(n * otile, otile), otile)
            one.part[:, columns] = dot(att[...], wo[:, columns]).astype(BF16)

        pad = jnp.zeros((seq_len, LANES - ao_ref.shape[0]), F32)
        one.part[:, width:] = jnp.concatenate([dot_t(att[...], ao_ref[...]), pad], 1).astype(BF16)

        @pl.when(c == 0)
        def _():
            gather.cross(1)

    def mlp_start(c):
        load_h(c).wait()
        keep = masks_ref[c, :, mixed:2 * mixed] > 0
        t_buf[...] = jnp.where(keep, dot_t(ubuf[...], full[1]).astype(BF16).astype(F32), 0.0).astype(BF16)

    def gate_up(c, begin, end):
        def product(w_ref, b_ref, j, side):
            copy, place = load_tile(w_ref, c, j, side)
            copy.wait()
            columns = pl.ds(pl.multiple_of(j * gtile, gtile), gtile)
            out = dot(ubuf[...], ring[place]) + scale * dot(t_buf[...], b_ref[:, columns])
            return out.astype(BF16)

        def refill(w_ref, j, side):
            wrap = j // pairs
            @pl.when(c + wrap < count)
            def _():
                load_tile(w_ref, c + wrap, j % pairs, side)[0].start()

        @pl.loop(begin, end)
        def _(j):
            columns = pl.ds(pl.multiple_of(j * gtile, gtile), gtile)
            mid[:, columns] = product(wg_ref, bg_ref, j, 0)
            refill(wu_ref, j + 1, 1)
            up = product(wu_ref, bu_ref, j, 1)
            refill(wg_ref, j + 2, 0)
            mid[:, columns] = (jax.nn.silu(mid[:, columns].astype(F32)) * up.astype(F32)).astype(BF16)

    def down(c):
        @pl.when(c + LAG + 1 < count)
        def _():
            load_x(c + LAG + 1).start()

        @pl.loop(0, downs)
        def _(n):
            @pl.when(c == 0)
            def _():
                load_d(n).wait()
            columns = pl.ds(pl.multiple_of(n * dtile, dtile), dtile)
            two.part[:, columns] = dot(mid[...], wd[n]).astype(BF16)

        pad = jnp.zeros((seq_len, LANES - ad_ref.shape[0]), F32)
        two.part[:, width:] = jnp.concatenate([dot_t(mid[...], ad_ref[...]), pad], 1).astype(BF16)

    def totals(c, total, exchange, first_b):
        tile = width // (mixed // own_ref.shape[1])
        lanes = total(0, exchange.rows, pl.ds(width, LANES)).astype(BF16).astype(F32)
        lane = lax.broadcasted_iota(jnp.int32, lanes.shape, 1)
        keep = masks_ref[c, :, 2 * mixed:2 * mixed + LANES] > 0
        lanes = jnp.where(keep, lanes, 0.0)
        columns = [jnp.sum(jnp.where(lane % rank == r, lanes, 0.0), axis=1, keepdims=True) for r in range(rank)]
        chosen = amask_ref[c] > 0
        for n in range(width // tile):
            lora = None
            for r in range(rank):
                b_all = full[1, n * own_ref.shape[1] + first_b:n * own_ref.shape[1] + first_b + 8,
                             r * tile:(r + 1) * tile].astype(F32)
                b_row = jnp.sum(jnp.where(chosen[:, :1], b_all, 0.0), axis=0, keepdims=True)
                lora = columns[r] * b_row if lora is None else lora + columns[r] * b_row
            yield pl.ds(n * tile, tile), total(0, exchange.rows, pl.ds(n * tile, tile)) + scale * lora

    def finish_one(c, total, done):
        load_r(c).wait()
        square = jnp.zeros((one.rows, 1), F32)
        for columns, z_out in totals(c, total, one, 16):
            x_one = (rbuf[c % 2, :, columns].astype(F32) + z_out).astype(BF16)
            x1[c, :, columns] = x_one
            x_one = x_one.astype(F32)
            square += jnp.sum(x_one * x_one, axis=1, keepdims=True)
        inv_rms = lax.rsqrt(square / width + RMS_EPS)
        for n in range(width // 512):
            columns = pl.ds(n * 512, 512)
            done[:, columns] = (x1[c, :, columns].astype(F32) * inv_rms * gain_m_ref[:, columns]).astype(BF16)

    def finish_two(c, total, done):
        for columns, z_out in totals(c, total, two, 24):
            done[:, columns] = (x1[c, :, columns].astype(F32) + z_out).astype(BF16)

    split = pairs // 2

    @pl.loop(0, count + 2 * LAG)
    def _(slot):
        late = slot - LAG
        busy = (slot >= LAG) & (slot < count + LAG)
        one.second_stages(slot, count, lambda c: load_r(c).start())

        @pl.when((slot >= count) & busy)
        def _():
            load_h(late).start()

        @pl.when(slot < count)
        def _():
            attention(slot)
            one.start(one.copy0(slot))

        two.first_stages(late - 1, count, finish_two)

        @pl.when(busy)
        def _():
            mlp_start(late)
            gate_up(late, 0, split)

        one.first_stages(slot, count, finish_one)

        @pl.when(busy)
        def _():
            gate_up(late, split, pairs)

        two.second_stages(late, count, lambda c: None)

        @pl.when(busy)
        def _():
            down(late)
            two.start(two.copy0(late))


def solution(mesh):
    act_spec = P('dp', None, None)
    w_head_spec = P(None, 'tp', None)
    w_out_spec = P('tp', None, None)
    w_col_spec = P(None, 'tp')
    w_row_spec = P('tp', None)
    a_rank_spec = P(None, None, 'tp')
    b_head_spec = P(None, None, 'tp', None)
    b_col_spec = P(None, None, 'tp')
    a_head_spec = P(None, 'tp', None, None)
    a_row_spec = P(None, 'tp', None)
    in_specs = (act_spec, P('dp'), P(None), P(None), w_head_spec, w_head_spec, w_head_spec, w_out_spec,
                w_col_spec, w_col_spec, w_row_spec, a_rank_spec, b_head_spec, a_rank_spec, b_head_spec,
                a_rank_spec, b_head_spec, a_head_spec, b_col_spec, a_rank_spec, b_col_spec,
                a_rank_spec, b_col_spec, a_row_spec, b_col_spec)

    def local_layer(x_in, adapter_ids, gain_attn, gain_mlp, w_q, w_k, w_v, w_o, w_gate, w_up, w_down,
                    a_q, b_q, a_k, b_k, a_v, b_v, a_o, b_o, a_gate, b_gate, a_up, b_up, a_down, b_down):
        count, seq_len, width = x_in.shape
        adapters, rank = b_q.shape[:2]
        mixed = adapters * rank
        scale = value_a10 / rank
        ff = w_gate.shape[1]

        group = mesh.shape['tp']
        head_dim = w_k.shape[2]
        n_q, n_k = w_q[0].size, w_k[0].size

        def plane(b):
            return b.transpose(1, 0, 2).reshape(group, adapters, -1)

        def planes(parts):
            zero = jnp.zeros_like(parts[0])
            return jnp.stack(list(parts) + [zero] * (4 - len(parts)), 1).reshape(4 * mixed, -1)

        a_loc = [a.transpose(2, 0, 1).reshape(adapters, width) for a in (a_q, a_k, a_v, a_gate, a_up)]
        b_loc = [b.reshape(adapters, -1) for b in (b_o, b_down)]
        own = jnp.stack([jnp.concatenate(a_loc[:3] + [jnp.zeros_like(a_loc[0])], 0),
                         jnp.concatenate(a_loc[3:] + b_loc, 0)])
        b_in = [plane(b.reshape(adapters, rank, -1)) for b in (b_q, b_k, b_v)]
        n_all = n_q + 2 * n_k
        b_qkv = planes([jnp.pad(b, ((0, 0), (0, 0), (at, n_all - at - b.shape[2])))
                        for b, at in zip(b_in, (0, n_q, n_q + n_k))])
        b_g = planes([plane(b_gate)])
        b_u = planes([jnp.zeros_like(plane(b_up)), plane(b_up)])

        index = jnp.arange(4 * mixed)
        mine = index % adapters == adapter_ids[:, None]
        index_plane = index // adapters % 4
        lane = jnp.arange(LANES)
        masks = jnp.concatenate([mine & (index_plane < 3), mine & (index_plane < 2),
                                 lane // rank == adapter_ids[:, None]], 1).astype(F32)
        amask = jnp.broadcast_to((jnp.arange(adapters) == adapter_ids[:, None])[:, :, None].astype(F32),
                                 (count, adapters, LANES))
        w_all = jnp.concatenate([w.reshape(width, -1) for w in (w_q, w_k, w_v)], 1)
        a_o_t = a_o.transpose(0, 3, 1, 2).reshape(mixed, -1)
        a_d_t = a_down.transpose(0, 2, 1).reshape(mixed, -1)

        gtile, dtile = 256, 1024
        dma = pltpu.SemaphoreType.DMA
        exchange_scratch = Exchange.scratch(seq_len, width + LANES, width)
        own_rows = seq_len // 2 // CHIPS
        out, _ = pl.pallas_call(
            functools.partial(layer_kernel, count, scale, rank, n_q // head_dim, head_dim),
            out_shape=(jax.ShapeDtypeStruct(x_in.shape, BF16), jax.ShapeDtypeStruct(x_in.shape, BF16)),
            in_specs=[ANY] * 6 + [VMEM] * 10, out_specs=(ANY, ANY),
            scratch_shapes=exchange_scratch * 2 + [pltpu.VMEM((2, 4 * mixed, width), BF16)] + Gather.scratch() + [
                pltpu.VMEM((width, n_all), BF16), pltpu.VMEM((n_q, width), BF16),
                pltpu.VMEM((width // dtile, ff, dtile), BF16), pltpu.VMEM((3, width, gtile), BF16),
                pltpu.VMEM((seq_len, width), BF16), pltpu.VMEM((seq_len, n_all), BF16),
                pltpu.VMEM((seq_len, n_q), BF16), pltpu.VMEM((seq_len, ff), BF16),
                pltpu.VMEM((seq_len, 4 * mixed), BF16), pltpu.VMEM((count, own_rows, width), BF16),
                pltpu.VMEM((2, own_rows, width), BF16), dma((2,)), dma((width // dtile,)), dma((3,)), dma, dma,
                dma((2,))],
            compiler_params=pltpu.CompilerParams(collective_id=0, has_side_effects=True, vmem_limit_bytes=VMEM_LIMIT),
        )(x_in, w_all, w_o.reshape(-1, width), w_gate, w_up, w_down, own, b_qkv, b_g, b_u, a_o_t, a_d_t, masks[:, None], amask,
          gain_attn.reshape(1, -1), gain_mlp.reshape(1, -1))
        return out

    return jax.shard_map(local_layer, mesh=mesh, in_specs=in_specs, out_specs=act_spec, check_vma=False)
```
